32 devices in a mesh: ep: 8 (over z, x), corner: 4 (over y, core).
Axes of the slice: x: 2, y: 2, z: 4, core: 2. Of those that a mesh axis runs over, the one named last changes fastest.
Arguments:
- required: float32 [8, 262144], P('corner', 'ep'), may hold values from -3 to 3
- arrival: float32 [8, 262144], P('corner', 'ep'), may hold values from -7.2 to 7.2
- hold_required: float32 [8, 262144], P('corner', 'ep'), may hold values from -5.4 to 5.4
- early_arrival: float32 [8, 262144], P('corner', 'ep'), may hold values from -3 to 3
- part_ids: int32 [262144], P('ep'), may hold values from 0 to 63
- bin_edges: int32 [512], replicated, may hold values from -4096 to -1, as said below
Outputs:
- part_hist: float32 [64, 8, 2, 512], P(None, 'corner')
- part_tns: float32 [64, 8, 2], P(None, 'corner')
- part_share: float32 [64], replicated
- tns: float32 [8, 2], P('corner')
- wns: float32 [8, 2], P('corner')
- worst: float32 [2, 262144], P(None, 'ep')
The draws below stay inside these ranges and needn't reach their ends.
Inputs may be any that keep to these rules, and one draw needn't show every extreme that they name: `bin_edges`: strictly increasing and negative; consecutive nodes differ by 1 to 8.
All inputs are finite; a program needn't handle non-finite values.
Results may differ from the reference program's by a relative error of at most 0.0003.
Values sent between devices are 32-bit elements; how exact they have to be, the bound alone decides.
No kernel may reach another device: no remote copies, remote signals or barrier semaphores. Data moves between devices by JAX's collectives and lax.ppermute only.
A program may use at most 64 MiB of HBM per device.

```python
import math
import jax
import jax.numpy as jnp
import numpy as np
from jax import lax

BINS = 512
GROUPS = 64
CORNERS = 8
ENDPOINTS = 262144


def rising(key, scale):
    position = jnp.arange(ENDPOINTS, dtype=jnp.float32) / ENDPOINTS
    factor = 1.0 + 2.0 * position
    values = scale * factor * jax.random.normal(key, (CORNERS, ENDPOINTS), jnp.float32)
    return jnp.clip(values, -18.0 * scale, 18.0 * scale)


def draw_arrival(key, part):
    return rising(jax.random.fold_in(key, 11), 0.4)


def draw_hold_required(key, part):
    return rising(jax.random.fold_in(key, 23), 0.3)


def draw_bin_edges(key, part):
    gaps = jax.random.randint(jax.random.fold_in(key, 37), (BINS,), 1, 9, jnp.int32)
    return (-jnp.cumsum(gaps)[::-1]).astype(jnp.int32)


def with_ends(result, rng, low, largest):
    spot = [jax.random.randint(jax.random.fold_in(rng, axis), (), 0, length) for axis, length in enumerate(result.shape)]
    longest = result.shape.index(max(result.shape))
    neighbour = spot[:longest] + [(spot[longest] + 1) % result.shape[longest]] + spot[longest + 1:]
    return result.at[tuple(spot)].set(low).at[tuple(neighbour)].set(largest)


def shard_levels(stream_key, dims, shards, least, top_value):
    loudness, own = 1.0, jax.random.fold_in(stream_key, 6)
    for dim, blocks in shards:
        steps = jnp.exp(jax.random.uniform(jax.random.fold_in(own, dim), (blocks,), jnp.float32, least / len(shards), top_value / len(shards)))
        loudness = loudness * jnp.repeat(steps, dims[dim] // blocks).reshape([-1 if axis == dim else 1 for axis in range(len(dims))])
    return loudness


def rank_bounds(amount, lean):
    weights = [(1 << 20) // math.isqrt(rank ** lean) + 1 for rank in range(1, amount + 1)]
    deviation = 1 + sum(weights) // (1 << 30)
    return np.cumsum(np.array([max(1, weight // deviation) for weight in weights]))


def ranked(own_key, dims, count, slope):
    listing = rank_bounds(count, slope)
    ticket = jax.random.randint(jax.random.fold_in(own_key, 1), dims, 0, int(listing[count - 1]))
    rank = jnp.searchsorted(jnp.asarray(listing, jnp.int32), ticket, side="right")
    return jax.random.permutation(jax.random.fold_in(own_key, 2), count)[rank].astype(jnp.int32)


def centred(stream_key, dims, deviation, limit, pieces=(), kind=jnp.bfloat16):
    level = shard_levels(stream_key, dims, pieces, -0.22, 0.18) if pieces else 1.0
    entries = jax.random.normal(stream_key, dims, jnp.float32) * deviation * level
    return jnp.minimum(jnp.maximum(entries, -limit), limit).astype(kind)


def setup_inputs(seed: int = 0) -> dict:
    splits = jax.random.split(jax.random.key(seed), 7)
    required = centred(splits[0], (CORNERS, ENDPOINTS), 0.5, 3.0, ((0, 4), (1, 8)), jnp.float32)
    arrival = draw_arrival(jax.random.fold_in(splits[6], 71), 0)
    hold_required = draw_hold_required(jax.random.fold_in(splits[6], 71), 0)
    early_arrival = centred(splits[3], (CORNERS, ENDPOINTS), 0.5, 3.0, ((0, 4), (1, 8)), jnp.float32)
    part_ids = with_ends(ranked(splits[4], (ENDPOINTS,), GROUPS, 1), jax.random.fold_in(splits[4], 3), 0, GROUPS - 1).astype(jnp.int32)
    bin_edges = draw_bin_edges(jax.random.fold_in(splits[6], 71), 0)
    return dict(required=required, arrival=arrival, hold_required=hold_required, early_arrival=early_arrival, part_ids=part_ids, bin_edges=bin_edges)


def node_tables(bin_edges):
    nodes = bin_edges.astype(jnp.float32) * 0.001
    upper = jnp.concatenate([nodes[1:], jnp.zeros((1,), jnp.float32)])
    lower = jnp.concatenate([nodes[:1] - 1.0, nodes[:-1]])
    return nodes, lower, upper


def weights_at(index, level, nodes, lower, upper):
    node = nodes[index]
    low = lower[index]
    high = upper[index]
    rise = (level - low) / (node - low)
    fall = (high - level) / (high - node)
    return jnp.maximum(jnp.minimum(rise, fall), 0.0)


def rounded(values):
    narrow = lax.optimization_barrier(values.astype(jnp.bfloat16))
    return narrow.astype(jnp.float32)


def histogram(slack, part_ids, nodes, lower, upper):
    level = jnp.clip(slack, nodes[0], 0.0)
    first = jnp.searchsorted(nodes, level, side="right").astype(jnp.int32) - 1
    first = jnp.clip(first, 0, BINS - 1).astype(jnp.int32)
    second = jnp.minimum(first + 1, BINS - 1).astype(jnp.int32)
    w_first = rounded(weights_at(first, level, nodes, lower, upper))
    w_second = rounded(jnp.where(first + 1 < BINS, weights_at(second, level, nodes, lower, upper), 0.0))
    total = jax.ops.segment_sum(w_first, part_ids * BINS + first, num_segments=GROUPS * BINS)
    total = total + jax.ops.segment_sum(w_second, part_ids * BINS + second, num_segments=GROUPS * BINS)
    return total.reshape(GROUPS, BINS)


def reference(required, arrival, hold_required, early_arrival, part_ids, bin_edges):
    nodes, lower, upper = node_tables(bin_edges)
    setup = required - arrival
    hold = early_arrival - hold_required

    def one_corner(pair):
        return jnp.stack([histogram(pair[0], part_ids, nodes, lower, upper), histogram(pair[1], part_ids, nodes, lower, upper)], axis=1)

    hists = lax.map(one_corner, (setup, hold))
    density = GROUPS * BINS / ENDPOINTS
    part_hist = jnp.transpose(hists, (1, 0, 2, 3)) * density
    neg_setup = jnp.minimum(setup, 0.0)
    neg_hold = jnp.minimum(hold, 0.0)
    share = GROUPS / ENDPOINTS
    part_setup = jax.ops.segment_sum(neg_setup.T, part_ids, num_segments=GROUPS)
    part_holdn = jax.ops.segment_sum(neg_hold.T, part_ids, num_segments=GROUPS)
    part_tns = jnp.stack([part_setup, part_holdn], axis=2) * share
    counts = jax.ops.segment_sum(jnp.ones(part_ids.shape, jnp.float32), part_ids, num_segments=GROUPS)
    part_share = counts * share
    tns = jnp.stack([jnp.sum(neg_setup, axis=1), jnp.sum(neg_hold, axis=1)], axis=1) * (1.0 / ENDPOINTS)
    wns = jnp.stack([jnp.min(setup, axis=1), jnp.min(hold, axis=1)], axis=1)
    worst = jnp.stack([jnp.min(setup, axis=0), jnp.min(hold, axis=0)], axis=0)
    return (part_hist, part_tns, part_share, tns, wns, worst)
```

```python
import functools
import jax
import jax.numpy as jnp
from jax import lax
from jax.experimental import pallas as pl
from jax.experimental.pallas import tpu as pltpu
from jax.sharding import PartitionSpec as P

GROUPS = 64
LANES = 128

def tables(bin_edges):
    bins = bin_edges.shape[0]
    q = bin_edges + 4096
    cells = jnp.arange(bins, dtype=jnp.int32)
    cell_of = q >> 3
    bit = jnp.left_shift(1, q & 7)
    base = jnp.sum((cell_of[None, :] < cells[:, None]).astype(jnp.int32), axis=1)
    bits = jnp.sum(jnp.where(cell_of[None, :] == cells[:, None], bit[None, :], 0), axis=1)
    coarse = base + bits * 65536
    nxt = jnp.concatenate([q[1:], jnp.full((1,), 4096, jnp.int32)])
    fine = q + (nxt - q) * 65536
    return coarse.reshape(-1, LANES), fine.reshape(-1, LANES)

def lookup(table_ref, index):
    lane = index & (LANES - 1)
    row = index >> 7
    out = None
    for r in range(table_ref.shape[0]):
        t = jnp.broadcast_to(table_ref[r:r + 1, :], index.shape)
        g = jnp.take_along_axis(t, lane, axis=1, mode="promise_in_bounds")
        out = g if out is None else jnp.where(row == r, g, out)
    return out

def dense(slack, coarse_ref, fine_ref, x0):
    t = jnp.minimum(jnp.maximum(slack, x0), 0.0)
    nf = jnp.floor(t * 1000.0)
    nf = jnp.where(t >= (nf + 1.0) * jnp.float32(0.001), nf + 1.0, nf)
    nf = jnp.where(t < nf * jnp.float32(0.001), nf - 1.0, nf)
    q = jnp.minimum(nf.astype(jnp.int32) + 4096, 4095)
    g = lookup(coarse_ref, q >> 3)
    low = jnp.left_shift(2, q & 7) - 1
    j = (g & 0xFFFF) + lax.population_count((g >> 16) & low) - 1
    f = lookup(fine_ref, j)
    k = (f & 0xFFFF) - 4096
    x = k.astype(jnp.float32) * jnp.float32(0.001)
    xn = (k + (f >> 16)).astype(jnp.float32) * jnp.float32(0.001)
    r = 1.0 / (xn - x)
    w1 = jnp.maximum((xn - t) * r, 0.0)
    w2 = jnp.maximum((t - x) * r, 0.0)
    jl = j & (LANES - 1)
    odd = (j & 1) == 1
    ce = ((jl + 1) & ~1).astype(jnp.float32)
    co = (jl | 1).astype(jnp.float32)
    we = jnp.where(odd, w2, w1)
    wo = jnp.where(odd, w1, w2)
    h = (j >> 7).astype(jnp.float32)
    return ce, co, we, wo, h, jnp.minimum(slack, 0.0)

def dense_kernel(C, x0_ref, coarse_ref, fine_ref, a_ref, b_ref, c_ref, d_ref, out_ref, worst_ref, low_ref):
    x0 = x0_ref[0]
    slacks = (a_ref[...] - b_ref[...], c_ref[...] - d_ref[...])
    for m, s in enumerate(slacks):
        for i, v in enumerate(dense(s, coarse_ref, fine_ref, x0)):
            out_ref[i, m] = v
    rows = slacks[0].shape[0]

    @pl.when(pl.program_id(0) == 0)
    def _():
        low_ref[...] = jnp.full_like(low_ref, jnp.inf)

    for m in range(2):
        folded = jnp.min(slacks[m].reshape(rows // 8, 8, LANES), axis=0)
        low_ref[m] = jnp.minimum(low_ref[m], folded)
    setup, hold = slacks
    even = (lax.broadcasted_iota(jnp.int32, setup.shape, 0) & 1) == 0
    worst_ref[...] = jnp.where(
        even,
        jnp.minimum(setup, pltpu.roll(setup, rows - 1, 0)),
        jnp.minimum(hold, pltpu.roll(hold, 1, 0)),
    )


def run_dense(req, arr, early, hreq, coarse, fine, x0, C):
    R = req.shape[0]
    blk = min(128, R)
    spec = pl.BlockSpec((blk, LANES), lambda i: (i, 0))
    tab = pl.BlockSpec(coarse.shape, lambda i: (0, 0))
    return pl.pallas_call(
        functools.partial(dense_kernel, C),
        grid=(R // blk,),
        in_specs=[pl.BlockSpec(memory_space=pltpu.SMEM), tab, tab, spec, spec, spec, spec],
        out_specs=[
            pl.BlockSpec((6, 2, blk, LANES), lambda i: (0, 0, i, 0)),
            spec,
            pl.BlockSpec((2, 8, LANES), lambda i: (0, 0, 0)),
        ],
        out_shape=[
            jax.ShapeDtypeStruct((6, 2, R, LANES), jnp.float32),
            jax.ShapeDtypeStruct((R, LANES), jnp.float32),
            jax.ShapeDtypeStruct((2, 8, LANES), jnp.float32),
        ],
        name="dense",
    )(x0, coarse, fine, req, arr, early, hreq)

NT = (((1,), (1,)), ((), ()))

def mm_kernel(C, KT, ids_ref, d_ref, low_ref, hist_ref, stat_ref, lbuf, rbuf, zbuf, pbuf, acc, sacc):
    step = pl.program_id(0)
    nblk = lbuf.shape[1] // GROUPS

    @pl.when(step == 0)
    def _():
        acc[...] = jnp.zeros_like(acc)
        sacc[...] = jnp.zeros_like(sacc)

    bf = jnp.bfloat16
    iota16 = lax.broadcasted_iota(jnp.int32, (16, LANES), 0)
    iotas = [(iota16 + 16 * v).astype(jnp.float32).astype(bf) for v in range(8)]
    even = (iota16 & 1) == 0
    iota8 = lax.broadcasted_iota(jnp.int32, (8, LANES), 0)
    one = jnp.ones((16, LANES), bf)
    zero = jnp.zeros((16, LANES), bf)
    tail = jnp.where(iota8 == 7, 1.0, 0.0)

    def row16(ref, *idx):
        return jnp.broadcast_to(ref[idx], (16, LANES))

    for k in range(KT):
        sl = slice(k * LANES, (k + 1) * LANES)
        pr = row16(ids_ref, slice(k, k + 1), slice(None)).astype(jnp.float32).astype(bf)
        lp = [jnp.where(iotas[v] == pr, one, zero) for v in range(GROUPS // 16)]
        for v in range(GROUPS // 16):
            pbuf[16 * v:16 * v + 16, sl] = lp[v]
        for c in range(C):
            zs = []
            for m in range(2):
                s = c * 2 + m
                r = k * C + c
                get = lambda q: d_ref[q, m, r:r + 1, :]
                b16 = lambda x: jnp.broadcast_to(x, (16, LANES))
                ce, co, we, wo = b16(get(0)), b16(get(1)), b16(get(2)), b16(get(3))
                hr = b16(get(4)).astype(bf)
                idx = jnp.where(even, ce, co).astype(bf)
                w = jnp.where(even, we, wo).astype(bf)
                for v in range(8):
                    rbuf[s, 16 * v:16 * v + 16, sl] = jnp.where(iotas[v] == idx, w, zero)
                for b in range(nblk):
                    mh = hr == jnp.bfloat16(b)
                    for v in range(GROUPS // 16):
                        o = b * GROUPS + 16 * v
                        lbuf[s, o:o + 16, sl] = jnp.where(mh, lp[v], zero)
                b8 = lambda x: jnp.broadcast_to(x, (8, LANES))
                neg, h8, ce8, we8 = b8(get(5)), b8(get(4)), b8(get(0)), b8(get(2))
                hi = neg.astype(bf).astype(jnp.float32)
                cross = jnp.where(ce8 == float(LANES), we8, 0.0)
                z = jnp.where(h8 + 2.0 == iota8.astype(jnp.float32), cross, tail)
                z = jnp.where(iota8 == 0, hi, jnp.where(iota8 == 1, neg - hi, z))
                zs.append(z)
            zbuf[16 * c:16 * c + 16, sl] = jnp.concatenate(zs, axis=0).astype(bf)
    for s in range(2 * C):
        acc[s] += lax.dot_general(lbuf[s], rbuf[s], NT, preferred_element_type=jnp.float32)
    sacc[...] += lax.dot_general(pbuf[...], zbuf[...], NT, preferred_element_type=jnp.float32)

    @pl.when(step == pl.num_programs(0) - 1)
    def _():
        stats = sacc[...]
        lane = lax.broadcasted_iota(jnp.int32, (GROUPS, LANES), 1)
        width = 2 * C * nblk
        out = jnp.concatenate([stats, jnp.zeros((GROUPS, LANES - 16 * C), jnp.float32)], axis=1)
        for c in range(C):
            for m in range(2):
                s = c * 2 + m
                rows8 = lax.broadcasted_iota(jnp.int32, (8, LANES), 0)
                low = jnp.min(jnp.where(rows8 % C == c, low_ref[m], jnp.inf), keepdims=True)
                out = jnp.where(lane == 16 * C + s, low, out)
                for b in range(nblk):
                    value = acc[s, b * GROUPS:(b + 1) * GROUPS, :]
                    if b:
                        column = stats[:, s * 8 + 1 + b:s * 8 + 2 + b]
                        value = jnp.where(lane == 0, value + column, value)
                    hist_ref[pl.ds((c * nblk + b) * 2 + m, GROUPS, stride=width), :] = value
        stat_ref[...] = out

def run_mm(ids, planes, low, C, KT=8):
    LT = ids.shape[0]
    bins_rows = 4 * GROUPS
    K = KT * LANES
    return pl.pallas_call(
        functools.partial(mm_kernel, C, KT),
        grid=(LT // KT,),
        in_specs=[pl.BlockSpec((KT, LANES), lambda i: (i, 0)),
                  pl.BlockSpec((6, 2, KT * C, LANES), lambda i: (0, 0, i, 0)),
                  pl.BlockSpec((2, 8, LANES), lambda i: (0, 0, 0))],
        out_specs=[pl.BlockSpec((2 * C * bins_rows, LANES), lambda i: (0, 0)),
                   pl.BlockSpec((GROUPS, LANES), lambda i: (0, 0))],
        out_shape=[jax.ShapeDtypeStruct((2 * C * bins_rows, LANES), jnp.float32),
                   jax.ShapeDtypeStruct((GROUPS, LANES), jnp.float32)],
        scratch_shapes=[pltpu.VMEM((2 * C, bins_rows, K), jnp.bfloat16),
                        pltpu.VMEM((2 * C, LANES, K), jnp.bfloat16),
                        pltpu.VMEM((16 * C, K), jnp.bfloat16),
                        pltpu.VMEM((GROUPS, K), jnp.bfloat16),
                        pltpu.VMEM((2 * C, bins_rows, LANES), jnp.float32),
                        pltpu.VMEM((GROUPS, 16 * C), jnp.float32)],
        name="mm",
    )(ids, planes, low)


def rotate(value, axis, distance):
    size = lax.axis_size(axis)
    return lax.ppermute(value, axis, [(i, (i + distance) % size) for i in range(size)])


def tiles(x):
    c, e = x.shape
    return x.reshape(c, e // LANES, LANES).transpose(1, 0, 2).reshape(-1, LANES)


def on_device(required, arrival, hold_required, early_arrival, part_ids, bin_edges):
    C, rows = required.shape
    bins = bin_edges.shape[0]
    n = lax.axis_size("ep")
    me = lax.axis_index("ep")
    endpoints = rows * n
    density = GROUPS * bins / endpoints
    share = GROUPS / endpoints
    x0 = bin_edges[:1].astype(jnp.float32) * jnp.float32(0.001)
    coarse, fine = tables(bin_edges)
    planes, near, low = run_dense(
        tiles(required), tiles(arrival), tiles(early_arrival), tiles(hold_required), coarse, fine, x0, C
    )
    worst = near
    for d in range(1, lax.axis_size("corner")):
        worst = jnp.minimum(worst, rotate(near, "corner", d))
    worst = worst.reshape(rows // LANES, 2, LANES).transpose(1, 0, 2).reshape(2, rows)

    hist, stat = run_mm(part_ids.reshape(-1, LANES), planes, low, C)
    own = GROUPS // n
    pad = -own % 8
    nblk = bins // LANES
    hrows = own * 2 * C * nblk
    stat = jnp.pad(stat.reshape(n, own, LANES), ((0, 0), (0, pad), (0, 0)))
    chunk = jnp.concatenate([hist.reshape(n, hrows, LANES), stat], axis=1)
    lanes = lax.broadcasted_iota(jnp.int32, (own + pad, LANES), 1)
    total = lax.dynamic_index_in_dim(chunk, me, 0, False)
    hsum, ssum = total[:hrows], total[hrows:]
    for d in range(1, n):
        got = rotate(lax.dynamic_index_in_dim(chunk, (me + d) % n, 0, False), "ep", d)
        hsum = hsum + got[:hrows]
        ssum = jnp.where(lanes >= 16 * C, jnp.minimum(ssum, got[hrows:]), ssum + got[hrows:])
    mine = jnp.concatenate([hsum * density, ssum], axis=0)
    full = jnp.zeros((n, hrows, LANES), jnp.float32)
    sfull = jnp.zeros((n, own + pad, LANES), jnp.float32)
    for d in range(n):
        got = rotate(mine, "ep", d) if d else mine
        full = lax.dynamic_update_index_in_dim(full, got[:hrows], (me - d) % n, 0)
        sfull = lax.dynamic_update_index_in_dim(sfull, got[hrows:], (me - d) % n, 0)
    part_hist = (
        full.reshape(GROUPS, C, nblk, 2, LANES).transpose(0, 1, 3, 2, 4).reshape(GROUPS, C, 2, bins)
    )
    stats = sfull[:, :own].reshape(GROUPS, LANES)
    cols = stats[:, :16 * C].reshape(GROUPS, C, 2, 8)
    sums = cols[..., 0] + cols[..., 1]
    part_tns = sums * share
    part_share = cols[:, 0, 0, 7] * share
    tns = jnp.sum(sums, axis=0) * (1.0 / endpoints)
    wns = stats[0, 16 * C:18 * C].reshape(C, 2)
    return (part_hist, part_tns, part_share, tns, wns, worst)


def solution(mesh):
    in_specs = (
        P("corner", "ep"),
        P("corner", "ep"),
        P("corner", "ep"),
        P("corner", "ep"),
        P("ep"),
        P(),
    )
    out_specs = (
        P(None, "corner", None, None),
        P(None, "corner", None),
        P(),
        P("corner", None),
        P("corner", None),
        P(None, "ep"),
    )
    return jax.shard_map(
        on_device, mesh=mesh, in_specs=in_specs, out_specs=out_specs, check_vma=False
    )
```

```python
import functools
import jax
import jax.numpy as jnp
from jax import lax
from jax.experimental import pallas as pl
from jax.experimental.pallas import tpu as pltpu
from jax.sharding import PartitionSpec as P

GROUPS = 64
LANES = 128
LEAST = 4096
F8 = jnp.float8_e4m3fn
BF = jnp.bfloat16
STEP = 0.001


def lookup(table_ref, index):
    lane = index & (LANES - 1)
    row = index >> 7
    out = None
    for r in range(table_ref.shape[0]):
        line = jnp.broadcast_to(table_ref[r:r + 1, :], index.shape)
        got = jnp.take_along_axis(line, lane, axis=1, mode="promise_in_bounds")
        out = got if out is None else jnp.where(row == r, got, out)
    return out


def interval(slack, x0, coarse_ref, fine_ref):
    t = jnp.minimum(jnp.maximum(slack, x0), 0.0)
    whole = jnp.floor(t * 1000.0)
    whole = jnp.where(t >= (whole + 1.0) * jnp.float32(STEP), whole + 1.0, whole)
    whole = jnp.where(t < whole * jnp.float32(STEP), whole - 1.0, whole)
    q = jnp.minimum(whole.astype(jnp.int32) + LEAST, LEAST - 1)
    cell = lookup(coarse_ref, q >> 3)
    upto = jnp.left_shift(2, q & 7) - 1
    j = (cell & 0xFFFF) + lax.population_count((cell >> 16) & upto) - 1
    pair = lookup(fine_ref, j)
    k = (pair & 0xFFFF) - LEAST
    x = k.astype(jnp.float32) * jnp.float32(STEP)
    xn = (k + (pair >> 16)).astype(jnp.float32) * jnp.float32(STEP)
    r = 1.0 / (xn - x)
    w1 = jnp.maximum((xn - t) * r, 0.0)
    w2 = jnp.maximum((t - x) * r, 0.0)
    local = j & (LANES - 1)
    odd = (j & 1) == 1
    even_place = ((local + 1) & ~1).astype(jnp.float32)
    odd_place = (local | 1).astype(jnp.float32)
    return (
        even_place,
        odd_place,
        jnp.where(odd, w2, w1),
        jnp.where(odd, w1, w2),
        (j >> 7).astype(jnp.float32),
        jnp.minimum(slack, 0.0),
    )


def prep_kernel(C, edges_ref, lines_ref, a_ref, b_ref, c_ref, d_ref, coarse_ref, fine_ref, worst_ref, low_ref):
    bins = edges_ref.shape[0]
    cell = lax.broadcasted_iota(jnp.int32, coarse_ref.shape, 0) * LANES + lax.broadcasted_iota(
        jnp.int32, coarse_ref.shape, 1
    )
    zero = jnp.zeros(coarse_ref.shape, jnp.int32)

    def add(i, state):
        state = list(state)
        for u in range(16):
            q = edges_ref[i * 16 + u] + LEAST
            here = q >> 3
            base, bits = state[u % 4]
            base = base + jnp.where(cell > here, 1, 0)
            bits = bits + jnp.where(cell == here, jnp.left_shift(65536, q & 7), 0)
            state[u % 4] = (base, bits)
        return tuple(state)

    state = lax.fori_loop(0, bins // 16, add, tuple((zero, zero) for _ in range(4)))
    coarse_ref[...] = sum(base + bits for base, bits in state)
    q = lines_ref[...] + LEAST
    _, lanes = q.shape
    left = pltpu.roll(q, lanes - 1, 1)
    below = jnp.concatenate([left[1:], jnp.full((1, lanes), LEAST, jnp.int32)], axis=0)
    last = lax.broadcasted_iota(jnp.int32, q.shape, 1) == lanes - 1
    following = jnp.where(last, below, left)
    fine_ref[...] = q + (following - q) * 65536

    setup = a_ref[...] - b_ref[...]
    hold = c_ref[...] - d_ref[...]
    size = setup.shape[0]
    for m, slack in enumerate((setup, hold)):
        low_ref[m] = jnp.min(slack.reshape(size // 8, 8, LANES), axis=0)
    first = lax.broadcasted_iota(jnp.int32, setup.shape, 0) % C == 0
    for m, slack in enumerate((setup, hold)):
        least = slack
        for c in range(1, C):
            least = jnp.minimum(least, pltpu.roll(slack, size - c, 0))
        if m:
            least = pltpu.roll(least, 1, 0)
            worst_ref[...] = jnp.where(first, worst_ref[...], least)
        else:
            worst_ref[...] = least


def run_prep(edges, a, b, c, d, C):
    bins = edges.shape[0]
    return pl.pallas_call(
        functools.partial(prep_kernel, C),
        in_specs=[pl.BlockSpec(memory_space=pltpu.SMEM)] + [pl.BlockSpec(memory_space=pltpu.VMEM)] * 5,
        out_shape=[
            jax.ShapeDtypeStruct((LEAST // 8 // LANES, LANES), jnp.int32),
            jax.ShapeDtypeStruct((bins // LANES, LANES), jnp.int32),
            jax.ShapeDtypeStruct(a.shape, jnp.float32),
            jax.ShapeDtypeStruct((2, 8, LANES), jnp.float32),
        ],
        name="prep",
    )(edges, edges.reshape(-1, LANES), a, b, c, d)


def hist_kernel(C, KT, n, edges_ref, coarse_ref, fine_ref, ids_ref, a_ref, b_ref, c_ref, d_ref, low_ref, out_ref, buf0, buf1):
    series = 2 * C
    nblk = fine_ref.shape[0]
    lines = KT * C
    chunks = ids_ref.shape[0] // KT
    own = GROUPS // n
    x0 = edges_ref[0].astype(jnp.float32) * jnp.float32(STEP)

    def body(*accs):
        for a in accs:
            pltpu.matmul_pop(a)
        iota16 = lax.broadcasted_iota(jnp.int32, (16, LANES), 0)
        iotas = [(iota16 + 16 * v).astype(jnp.float32).astype(BF) for v in range(LANES // 16)]
        iota32 = lax.broadcasted_iota(jnp.int32, (32, LANES), 0)
        iotas32 = [(iota32 + 32 * v).astype(jnp.float32).astype(BF) for v in range(GROUPS // 32)]
        even = (iota16 & 1) == 0
        iota8 = lax.broadcasted_iota(jnp.int32, (8, LANES), 0)
        one = jnp.ones((32, LANES), BF)
        zero16 = jnp.zeros((16, LANES), BF)
        zero32 = jnp.zeros((32, LANES), BF)
        none = jnp.zeros((32, LANES), F8)
        tail = jnp.where(iota8 == 3, 1.0, 0.0)

        def wide(x, rows):
            return jnp.broadcast_to(x, (rows, LANES))

        def look(buf, chunk, g):
            start = pl.multiple_of(chunk * lines + g * 8, 8)
            at = pl.ds(start, 8)
            for m, slack in enumerate((a_ref[at, :] - b_ref[at, :], c_ref[at, :] - d_ref[at, :])):
                for i, v in enumerate(interval(slack, x0, coarse_ref, fine_ref)):
                    buf[i, m, g * 8:g * 8 + 8, :] = v

        def pair(buf, chunk, k2):
            member = []
            for kk in range(2):
                ids = wide(ids_ref[pl.ds(chunk * KT + 2 * k2 + kk, 1), :], 32).astype(jnp.float32).astype(BF)
                member.append([jnp.where(i == ids, one, zero32).astype(F8) for i in iotas32])
            for s in range(series):
                c, m = divmod(s, 2)
                left, right = [], []
                for kk in range(2):
                    r = (2 * k2 + kk) * C + c
                    row = [buf[i, m, r:r + 1, :] for i in range(6)]
                    block = wide(row[4], 32).astype(BF)
                    left.append(jnp.concatenate([
                        jnp.where(block == jnp.bfloat16(h), part, none) for h in range(nblk) for part in member[kk]
                    ], axis=0))
                    place = jnp.where(even, wide(row[0], 16), wide(row[1], 16)).astype(BF)
                    weight = jnp.where(even, wide(row[2], 16), wide(row[3], 16)).astype(BF)
                    hats = [jnp.where(i == place, weight, zero16) for i in iotas]
                    negative = wide(row[5], 8)
                    high = negative.astype(BF).astype(jnp.float32)
                    cross = jnp.where(wide(row[0], 8) == float(LANES), wide(row[2], 8), 0.0)
                    z = jnp.where(iota8 == 2, cross, tail)
                    z = jnp.where(iota8 == 0, high, jnp.where(iota8 == 1, negative - high, z))
                    hats.append(jnp.concatenate([z, jnp.zeros((8, LANES), jnp.float32)], axis=0).astype(BF))
                    right.append(jnp.concatenate(hats, axis=0))
                pltpu.matmul_push_rhs(
                    jnp.concatenate(left, axis=1), staging_register=0, mxu_index=s % 2, transpose=True
                )
                pltpu.matmul_acc_lhs(accs[s], jnp.concatenate(right, axis=1), load_staged_rhs=0)

        def both(chunk, buf, ahead, other):
            pairs, groups = KT // 2, lines // 8
            done = 0
            for k2 in range(pairs):
                pair(buf, chunk, k2)
                while done < groups and done * pairs <= k2 * groups:
                    look(other, ahead, done)
                    done += 1

        for g in range(lines // 8):
            look(buf0, 0, g)

        def two(i, carry):
            both(2 * i, buf0, 2 * i + 1, buf1)
            both(2 * i + 1, buf1, jnp.minimum(2 * i + 2, chunks - 1), buf0)
            return carry

        lax.fori_loop(0, chunks // 2, two, 0)

        stats, lane = [], lax.broadcasted_iota(jnp.int32, (GROUPS, LANES), 1)
        sums = [pltpu.matmul_pop(a) for a in accs]
        for out in sums:
            stats.append(out[LANES:])
        stats.append(jnp.zeros((LANES - 16 * series, nblk * GROUPS), jnp.float32))
        turned = jnp.concatenate(stats, axis=0).T
        total = sum(turned[h * GROUPS:(h + 1) * GROUPS] for h in range(nblk))
        sub8 = lax.broadcasted_iota(jnp.int32, (8, LANES), 0)
        chunk_rows = out_ref.shape[0] // n
        hist_rows = own * series * nblk
        for s in range(series):
            c, m = divmod(s, 2)
            low = jnp.min(jnp.where(sub8 % C == c, low_ref[m], jnp.inf), keepdims=True)
            total = jnp.where(lane == 16 * series + s, low, total)
            full = sums[s][:LANES].T
            for h in range(nblk):
                value = full[h * GROUPS:(h + 1) * GROUPS]
                if h:
                    column = turned[(h - 1) * GROUPS:h * GROUPS, 16 * s + 2:16 * s + 3]
                    value = jnp.where(lane == 0, value + column, value)
                for i in range(n):
                    at = i * chunk_rows + (c * nblk + h) * 2 + m
                    out_ref[pl.ds(at, own, stride=series * nblk), :] = value[i * own:(i + 1) * own]
        for i in range(n):
            at = i * chunk_rows + hist_rows
            out_ref[at:at + own, :] = total[i * own:(i + 1) * own]

    pl.run_scoped(body, *[pltpu.ACC(s % 2)((LANES + 16, 256), jnp.float32) for s in range(series)])


def run_hist(edges, coarse, fine, ids, a, b, c, d, low, C, n, KT=16):
    nblk = fine.shape[0]
    own = GROUPS // n
    rows = own * 2 * C * nblk + own + (-own % 8)
    vm = pl.BlockSpec(memory_space=pltpu.VMEM)
    return pl.pallas_call(
        functools.partial(hist_kernel, C, KT, n),
        in_specs=[pl.BlockSpec(memory_space=pltpu.SMEM)] + [vm] * 8,
        out_shape=jax.ShapeDtypeStruct((n * rows, LANES), jnp.float32),
        scratch_shapes=[pltpu.VMEM((6, 2, KT * C, LANES), jnp.float32) for _ in range(2)],
        cost_estimate=pl.CostEstimate(
            flops=4 * C * (LANES + 16) * 256 * ids.size, bytes_accessed=16 * a.size, transcendentals=2 * a.size
        ),
        name="hist",
    )(edges, coarse, fine, ids, a, b, c, d, low)


def small_kernel(C, share, scale, stats_ref, part_ref, share_ref, tns_ref, wns_ref):
    turned = stats_ref[...].T
    tns = jnp.zeros((C, 2), jnp.float32)
    wns = jnp.zeros((C, 2), jnp.float32)
    row = lax.broadcasted_iota(jnp.int32, (C, 2), 0)
    col = lax.broadcasted_iota(jnp.int32, (C, 2), 1)
    for s in range(2 * C):
        c, m = divmod(s, 2)
        sums = turned[16 * s:16 * s + 1, :] + turned[16 * s + 1:16 * s + 2, :]
        part_ref[c, m:m + 1, :] = sums * share
        here = (row == c) & (col == m)
        tns = jnp.where(here, jnp.sum(sums, keepdims=True) * scale, tns)
        wns = jnp.where(here, turned[32 * C + s:32 * C + s + 1, :1], wns)
    share_ref[...] = turned[3:4, :] * share
    tns_ref[...] = tns
    wns_ref[...] = wns


def run_small(stats, C, endpoints):
    return pl.pallas_call(
        functools.partial(small_kernel, C, GROUPS / endpoints, 1.0 / endpoints),
        out_shape=[
            jax.ShapeDtypeStruct((C, 2, GROUPS), jnp.float32),
            jax.ShapeDtypeStruct((1, GROUPS), jnp.float32),
            jax.ShapeDtypeStruct((C, 2), jnp.float32),
            jax.ShapeDtypeStruct((C, 2), jnp.float32),
        ],
        name="small",
    )(stats)


def rotate(value, axis, distance):
    size = lax.axis_size(axis)
    return lax.ppermute(value, axis, [(i, (i + distance) % size) for i in range(size)])


def tiles(x):
    c, e = x.shape
    return x.reshape(c, e // LANES, LANES).transpose(1, 0, 2).reshape(-1, LANES)


def on_device(required, arrival, hold_required, early_arrival, part_ids, bin_edges):
    C, rows = required.shape
    bins = bin_edges.shape[0]
    n = lax.axis_size("ep")
    me = lax.axis_index("ep")
    endpoints = rows * n
    density = GROUPS * bins / endpoints
    series = 2 * C
    data = (tiles(required), tiles(arrival), tiles(early_arrival), tiles(hold_required))
    coarse, fine, near, low = run_prep(bin_edges, *data, C)
    shares = [rotate(near, "corner", d) for d in range(1, lax.axis_size("corner"))]
    chunks = run_hist(bin_edges, coarse, fine, part_ids.reshape(-1, LANES), *data, low, C, n)
    worst = functools.reduce(jnp.minimum, shares, near).reshape(rows // LANES, C, LANES)[:, :2]
    worst = worst.transpose(1, 0, 2).reshape(2, rows)

    own = GROUPS // n
    hrows = own * series * (bins // LANES)
    chunks = chunks.reshape(n, -1, LANES)
    total = lax.dynamic_index_in_dim(chunks, me, 0, False)
    lanes = lax.broadcasted_iota(jnp.int32, total[hrows:].shape, 1)
    hsum, ssum = total[:hrows], total[hrows:]
    for d in range(1, n):
        got = rotate(lax.dynamic_index_in_dim(chunks, (me + d) % n, 0, False), "ep", d)
        hsum = hsum + got[:hrows]
        ssum = jnp.where(lanes >= 16 * series, jnp.minimum(ssum, got[hrows:]), ssum + got[hrows:])
    mine = jnp.concatenate([hsum * density, ssum], axis=0)
    full = jnp.zeros((n, hrows, LANES), jnp.float32)
    sfull = jnp.zeros((n,) + ssum.shape, jnp.float32)
    for d in range(n):
        got = rotate(mine, "ep", d) if d else mine
        full = lax.dynamic_update_index_in_dim(full, got[:hrows], (me - d) % n, 0)
        sfull = lax.dynamic_update_index_in_dim(sfull, got[hrows:], (me - d) % n, 0)
    part_hist = (
        full.reshape(GROUPS, C, bins // LANES, 2, LANES).transpose(0, 1, 3, 2, 4).reshape(GROUPS, C, 2, bins)
    )
    stats = sfull[:, :own].reshape(GROUPS, LANES)
    part_tns, part_share, tns, wns = run_small(stats, C, endpoints)
    part_tns = part_tns.transpose(2, 0, 1)
    part_share = part_share.reshape(GROUPS)
    return (part_hist, part_tns, part_share, tns, wns, worst)


def solution(mesh):
    in_specs = (
        P("corner", "ep"),
        P("corner", "ep"),
        P("corner", "ep"),
        P("corner", "ep"),
        P("ep"),
        P(),
    )
    out_specs = (
        P(None, "corner", None, None),
        P(None, "corner", None),
        P(),
        P("corner", None),
        P("corner", None),
        P(None, "ep"),
    )
    return jax.shard_map(
        on_device, mesh=mesh, in_specs=in_specs, out_specs=out_specs, check_vma=False
    )
```

```python
import functools
import jax
import jax.numpy as jnp
from jax import lax
from jax.experimental import pallas as pl
from jax.experimental.pallas import tpu as pltpu
from jax.sharding import PartitionSpec as P

GROUPS = 64
LANES = 128
LEAST = 4096
F8 = jnp.float8_e4m3fn
BF = jnp.bfloat16
STEP = 0.001


def lookup(table_ref, index):
    lane = index & (LANES - 1)
    row = index >> 7
    out = None
    for r in range(table_ref.shape[0]):
        line = jnp.broadcast_to(table_ref[r:r + 1, :], index.shape)
        got = jnp.take_along_axis(line, lane, axis=1, mode="promise_in_bounds")
        out = got if out is None else jnp.where(row == r, got, out)
    return out


def interval(slack, x0, coarse_ref, fine_ref):
    t = jnp.minimum(jnp.maximum(slack, x0), 0.0)
    whole = jnp.floor(t * 1000.0)
    whole = jnp.where(t >= (whole + 1.0) * jnp.float32(STEP), whole + 1.0, whole)
    whole = jnp.where(t < whole * jnp.float32(STEP), whole - 1.0, whole)
    q = jnp.minimum(whole.astype(jnp.int32) + LEAST, LEAST - 1)
    cell = lookup(coarse_ref, q >> 3)
    upto = jnp.left_shift(2, q & 7) - 1
    j = (cell & 0xFFFF) + lax.population_count((cell >> 16) & upto) - 1
    pair = lookup(fine_ref, j)
    k = (pair & 0xFFFF) - LEAST
    x = k.astype(jnp.float32) * jnp.float32(STEP)
    xn = (k + (pair >> 16)).astype(jnp.float32) * jnp.float32(STEP)
    r = 1.0 / (xn - x)
    w1 = jnp.maximum((xn - t) * r, 0.0)
    w2 = jnp.maximum((t - x) * r, 0.0)
    local = j & (LANES - 1)
    odd = (j & 1) == 1
    even_place = ((local + 1) & ~1).astype(jnp.float32)
    odd_place = (local | 1).astype(jnp.float32)
    return (
        even_place,
        odd_place,
        jnp.where(odd, w2, w1),
        jnp.where(odd, w1, w2),
        (j >> 7).astype(jnp.float32),
        jnp.minimum(slack, 0.0),
    )


def prep_kernel(
    C, edges_ref, side_ref, lines_ref, ids_ref, a_ref, b_ref, c_ref, d_ref,
    coarse_ref, fine_ref, worst_ref, keep_ref, send_ref,
):
    bins = edges_ref.shape[0]
    cell = lax.broadcasted_iota(jnp.int32, coarse_ref.shape, 0) * LANES + lax.broadcasted_iota(
        jnp.int32, coarse_ref.shape, 1
    )
    zero = jnp.zeros(coarse_ref.shape, jnp.int32)

    def add(i, state):
        state = list(state)
        for u in range(16):
            q = edges_ref[i * 16 + u] + LEAST
            here = q >> 3
            base, bits = state[u % 4]
            base = base + jnp.where(cell > here, 1, 0)
            bits = bits + jnp.where(cell == here, jnp.left_shift(65536, q & 7), 0)
            state[u % 4] = (base, bits)
        return tuple(state)

    state = lax.fori_loop(0, bins // 16, add, tuple((zero, zero) for _ in range(4)))
    coarse_ref[...] = sum(base + bits for base, bits in state)
    q = lines_ref[...] + LEAST
    _, lanes = q.shape
    left = pltpu.roll(q, lanes - 1, 1)
    below = jnp.concatenate([left[1:], jnp.full((1, lanes), LEAST, jnp.int32)], axis=0)
    last = lax.broadcasted_iota(jnp.int32, q.shape, 1) == lanes - 1
    following = jnp.where(last, below, left)
    fine_ref[...] = q + (following - q) * 65536

    flag = side_ref[0] == 0
    half = C // 2
    lines = a_ref.shape[0] // C
    for m, (late, early) in enumerate(((a_ref, b_ref), (c_ref, d_ref))):
        for k in range(half):
            pieces = []
            for c in (k, k + half):
                at = pl.ds(c, lines, stride=C)
                pieces.append(late[at, :] - early[at, :])
            keep_ref[m, pl.ds(k, lines, stride=half), :] = jnp.where(flag, pieces[0], pieces[1])
            send_ref[m, pl.ds(k, lines, stride=half), :] = jnp.where(flag, pieces[1], pieces[0])
            for piece in pieces:
                first = k == 0 and piece is pieces[0]
                at = pl.ds(m, lines, stride=2)
                worst_ref[at, :] = piece if first else jnp.minimum(worst_ref[at, :], piece)
    ids = ids_ref[...].astype(jnp.float32)
    keep_ref[2, :lines, :] = ids
    send_ref[2, :lines, :] = ids


def run_prep(edges, side, ids, a, b, c, d, C):
    bins = edges.shape[0]
    lines = ids.shape[0]
    smem = pl.BlockSpec(memory_space=pltpu.SMEM)
    return pl.pallas_call(
        functools.partial(prep_kernel, C),
        in_specs=[smem, smem] + [pl.BlockSpec(memory_space=pltpu.VMEM)] * 6,
        out_shape=[
            jax.ShapeDtypeStruct((LEAST // 8 // LANES, LANES), jnp.int32),
            jax.ShapeDtypeStruct((bins // LANES, LANES), jnp.int32),
            jax.ShapeDtypeStruct((2 * lines, LANES), jnp.float32),
            jax.ShapeDtypeStruct((3, lines * C // 2, LANES), jnp.float32),
            jax.ShapeDtypeStruct((3, lines * C // 2, LANES), jnp.float32),
        ],
        name="prep",
    )(edges, side, edges.reshape(-1, LANES), ids, a, b, c, d)


def hist_kernel(C, KT, n, edges_ref, place_ref, coarse_ref, fine_ref, slack_ref, *refs):
    if n:
        prior_ref, prior_low_ref = refs[:2]
        outs, (low_ref, buf0, buf1, all_ref) = refs[2:2 + n], refs[2 + n:]
    else:
        out_ref, low_ref, buf0, buf1 = refs
    series = 2 * C
    nblk = fine_ref.shape[0]
    lines = KT * C
    chunks = slack_ref.shape[1] // lines
    x0 = edges_ref[0].astype(jnp.float32) * jnp.float32(STEP)

    def body(*accs):
        for a in accs:
            pltpu.matmul_pop(a)
        iota16 = lax.broadcasted_iota(jnp.int32, (16, LANES), 0)
        iotas = [(iota16 + 16 * v).astype(jnp.float32).astype(BF) for v in range(LANES // 16)]
        iota32 = lax.broadcasted_iota(jnp.int32, (32, LANES), 0)
        iotas32 = [(iota32 + 32 * v).astype(jnp.float32).astype(BF) for v in range(GROUPS // 32)]
        even = (iota16 & 1) == 0
        iota8 = lax.broadcasted_iota(jnp.int32, (8, LANES), 0)
        one = jnp.ones((32, LANES), BF)
        zero16 = jnp.zeros((16, LANES), BF)
        zero32 = jnp.zeros((32, LANES), BF)
        none = jnp.zeros((32, LANES), F8)
        tail = jnp.where(iota8 == 3, 1.0, 0.0)

        def wide(x, rows):
            return jnp.broadcast_to(x, (rows, LANES))

        def look(buf, chunk, g):
            start = pl.multiple_of(chunk * lines + g * 8, 8)
            at = pl.ds(start, 8)
            for m in range(2):
                slack = slack_ref[m, at, :]
                low_ref[m] = jnp.minimum(low_ref[m], slack)
                for i, v in enumerate(interval(slack, x0, coarse_ref, fine_ref)):
                    buf[i, m, g * 8:g * 8 + 8, :] = v

        def pair(buf, chunk, k2):
            member = []
            for kk in range(2):
                ids = wide(slack_ref[2, pl.ds(chunk * KT + 2 * k2 + kk, 1), :], 32).astype(BF)
                member.append([jnp.where(i == ids, one, zero32).astype(F8) for i in iotas32])
            for s in range(series):
                c, m = divmod(s, 2)
                left, right = [], []
                for kk in range(2):
                    r = (2 * k2 + kk) * C + c
                    row = [buf[i, m, r:r + 1, :] for i in range(6)]
                    block = wide(row[4], 32).astype(BF)
                    left.append(jnp.concatenate([
                        jnp.where(block == jnp.bfloat16(h), part, none) for h in range(nblk) for part in member[kk]
                    ], axis=0))
                    place = jnp.where(even, wide(row[0], 16), wide(row[1], 16)).astype(BF)
                    weight = jnp.where(even, wide(row[2], 16), wide(row[3], 16)).astype(BF)
                    hats = [jnp.where(i == place, weight, zero16) for i in iotas]
                    negative = wide(row[5], 8)
                    high = negative.astype(BF).astype(jnp.float32)
                    cross = jnp.where(wide(row[0], 8) == float(LANES), wide(row[2], 8), 0.0)
                    z = jnp.where(iota8 == 2, cross, tail)
                    z = jnp.where(iota8 == 0, high, jnp.where(iota8 == 1, negative - high, z))
                    hats.append(jnp.concatenate([z, jnp.zeros((8, LANES), jnp.float32)], axis=0).astype(BF))
                    right.append(jnp.concatenate(hats, axis=0))
                pltpu.matmul_push_rhs(
                    jnp.concatenate(left, axis=1), staging_register=0, mxu_index=s % 2, transpose=True
                )
                pltpu.matmul_acc_lhs(accs[s], jnp.concatenate(right, axis=1), load_staged_rhs=0)

        def both(chunk, buf, ahead, other):
            pairs, groups = KT // 2, lines // 8
            done = 0
            for k2 in range(pairs):
                pair(buf, chunk, k2)
                while done < groups and done * pairs <= k2 * groups:
                    look(other, ahead, done)
                    done += 1

        low_ref[...] = prior_low_ref[...] if n else jnp.full(low_ref.shape, jnp.inf)
        for g in range(lines // 8):
            look(buf0, 0, g)

        def two(i, carry):
            both(2 * i, buf0, 2 * i + 1, buf1)
            both(2 * i + 1, buf1, jnp.minimum(2 * i + 2, chunks - 1), buf0)
            return carry

        lax.fori_loop(0, chunks // 2, two, 0)

        stats, lane = [], lax.broadcasted_iota(jnp.int32, (GROUPS, LANES), 1)
        sums = [pltpu.matmul_pop(a) for a in accs]
        if not n:
            for s in range(series):
                out_ref[s] = sums[s]
            return
        sums = [prior_ref[s] + sums[s] for s in range(series)]
        own = GROUPS // n
        for out in sums:
            stats.append(out[LANES:])
        stats.append(jnp.zeros((LANES - 16 * series, nblk * GROUPS), jnp.float32))
        turned = jnp.concatenate(stats, axis=0).T
        total = sum(turned[h * GROUPS:(h + 1) * GROUPS] for h in range(nblk))
        sub8 = lax.broadcasted_iota(jnp.int32, (8, LANES), 0)
        chunk_rows = all_ref.shape[0] // n
        hist_rows = own * series * nblk
        for s in range(series):
            c, m = divmod(s, 2)
            low = jnp.min(jnp.where(sub8 % C == c, low_ref[m], jnp.inf), keepdims=True)
            total = jnp.where(lane == 16 * series + s, low, total)
            full = sums[s][:LANES].T
            for h in range(nblk):
                value = full[h * GROUPS:(h + 1) * GROUPS]
                if h:
                    column = turned[(h - 1) * GROUPS:h * GROUPS, 16 * s + 2:16 * s + 3]
                    value = jnp.where(lane == 0, value + column, value)
                for i in range(n):
                    at = i * chunk_rows + (c * nblk + h) * 2 + m
                    all_ref[pl.ds(at, own, stride=series * nblk), :] = value[i * own:(i + 1) * own]
        for i in range(n):
            at = i * chunk_rows + hist_rows
            all_ref[at:at + own, :] = total[i * own:(i + 1) * own]
        for d in range(n):
            at = pl.multiple_of(lax.rem(place_ref[0] + d, n) * chunk_rows, 8)
            outs[d][...] = all_ref[pl.ds(at, chunk_rows), :]

    pl.run_scoped(body, *[pltpu.ACC(s % 2)((LANES + 16, 256), jnp.float32) for s in range(series)])


def run_hist(edges, place, coarse, fine, slack, C, n=0, prior=(), KT=16):
    nblk = fine.shape[0]
    series = 2 * C
    smem = pl.BlockSpec(memory_space=pltpu.SMEM)
    vm = pl.BlockSpec(memory_space=pltpu.VMEM)
    scratch = [pltpu.VMEM((6, 2, KT * C, LANES), jnp.float32) for _ in range(2)]
    low = jax.ShapeDtypeStruct((2, 8, LANES), jnp.float32)
    if n:
        own = GROUPS // n
        rows = own * series * nblk + own + (-own % 8)
        outs = [jax.ShapeDtypeStruct((rows, LANES), jnp.float32) for _ in range(n)]
        scratch += [pltpu.VMEM((2, 8, LANES), jnp.float32)] * 0 + [pltpu.VMEM((n * rows, LANES), jnp.float32)]
    else:
        outs = [jax.ShapeDtypeStruct((series, LANES + 16, nblk * GROUPS), jnp.float32)]
    return pl.pallas_call(
        functools.partial(hist_kernel, C, KT, n),
        in_specs=[smem, smem] + [vm] * (3 + len(prior)),
        out_shape=outs + [low],
        scratch_shapes=scratch,
        cost_estimate=pl.CostEstimate(
            flops=4 * (LANES + 16) * 256 * slack.size // 3, bytes_accessed=8 * slack.size, transcendentals=slack.size
        ),
        name="hist",
    )(edges, place, coarse, fine, slack, *prior)


def final_kernel(C, own, share, scale, me_ref, *refs):
    n = len(refs) - 6
    pieces = refs[:n]
    hist_ref, part_ref, share_ref, tns_ref, wns_ref, stats_ref = refs[n:]
    half = C // 2
    each = hist_ref.shape[0] // GROUPS // 2
    for d in range(n):
        source = lax.rem(me_ref[0] - d + n, n)
        place, side = source >> 1, source & 1
        for p in range(own):
            at = pl.multiple_of((place * own + p) * 2 * each + side * each, 8)
            hist_ref[pl.ds(at, each), :] = pieces[d][p * each:(p + 1) * each, :]
        stats_ref[side, pl.ds(place * own, own), :] = pieces[d][own * each:own * each + own, :]
    tns = jnp.zeros((C, 2), jnp.float32)
    wns = jnp.zeros((C, 2), jnp.float32)
    row = lax.broadcasted_iota(jnp.int32, (C, 2), 0)
    col = lax.broadcasted_iota(jnp.int32, (C, 2), 1)
    for side in range(2):
        turned = stats_ref[side].T
        for s in range(2 * half):
            c, m = divmod(s, 2)
            c += side * half
            sums = turned[16 * s:16 * s + 1, :] + turned[16 * s + 1:16 * s + 2, :]
            part_ref[c, m:m + 1, :] = sums * share
            here = (row == c) & (col == m)
            tns = jnp.where(here, jnp.sum(sums, keepdims=True) * scale, tns)
            wns = jnp.where(here, turned[32 * half + s:32 * half + s + 1, :1], wns)
    share_ref[...] = turned[3:4, :] * share
    tns_ref[...] = tns
    wns_ref[...] = wns


def run_final(me, pieces, C, own, rows, endpoints):
    vm = pl.BlockSpec(memory_space=pltpu.VMEM)
    return pl.pallas_call(
        functools.partial(final_kernel, C, own, GROUPS / endpoints, 1.0 / endpoints),
        in_specs=[pl.BlockSpec(memory_space=pltpu.SMEM)] + [vm] * len(pieces),
        out_shape=[
            jax.ShapeDtypeStruct((GROUPS * rows, LANES), jnp.float32),
            jax.ShapeDtypeStruct((C, 2, GROUPS), jnp.float32),
            jax.ShapeDtypeStruct((1, GROUPS), jnp.float32),
            jax.ShapeDtypeStruct((C, 2), jnp.float32),
            jax.ShapeDtypeStruct((C, 2), jnp.float32),
        ],
        scratch_shapes=[pltpu.VMEM((2, GROUPS, LANES), jnp.float32)],
        name="final",
    )(me, *pieces)


def rotate(value, axis, distance):
    size = lax.axis_size(axis)
    return lax.ppermute(value, axis, [(i, (i + distance) % size) for i in range(size)])


def tiles(x):
    c, e = x.shape
    return x.reshape(c, e // LANES, LANES).transpose(1, 0, 2).reshape(-1, LANES)


def on_device(required, arrival, hold_required, early_arrival, part_ids, bin_edges):
    C, rows = required.shape
    bins = bin_edges.shape[0]
    n = lax.axis_size("ep")
    me = lax.axis_index("ep")
    endpoints = rows * n
    density = GROUPS * bins / endpoints
    half = C // 2
    side = me % 2
    place = me // 2
    rest = n // 2
    data = (tiles(required), tiles(arrival), tiles(early_arrival), tiles(hold_required))
    ids = part_ids.reshape(-1, LANES)
    lines = ids.shape[0]
    coarse, fine, near, keep, send = run_prep(bin_edges, side.reshape(1), ids, *data, C)
    got = lax.ppermute(send, "ep", [(i, i ^ 1) for i in range(n)])
    shares = [rotate(near, "corner", d) for d in range(1, lax.axis_size("corner"))]
    prior = run_hist(bin_edges, place.reshape(1), coarse, fine, keep, half)
    chunks = run_hist(bin_edges, place.reshape(1), coarse, fine, got, half, rest, prior)
    worst = functools.reduce(jnp.minimum, shares, near).reshape(lines, 2, LANES)
    worst = worst.transpose(1, 0, 2).reshape(2, rows)

    own = GROUPS // rest
    nblk = bins // LANES
    each = C * nblk
    hrows = own * each
    total = chunks[0]
    lanes = lax.broadcasted_iota(jnp.int32, total[hrows:].shape, 1)
    hsum, ssum = total[:hrows], total[hrows:]
    for d in range(1, rest):
        piece = rotate(chunks[d], "ep", 2 * d)
        hsum = hsum + piece[:hrows]
        ssum = jnp.where(lanes >= 32 * half, jnp.minimum(ssum, piece[hrows:]), ssum + piece[hrows:])
    mine = jnp.concatenate([hsum * density, ssum], axis=0)
    pieces = [rotate(mine, "ep", d) if d else mine for d in range(n)]
    full, part_tns, part_share, tns, wns = run_final(me.reshape(1), pieces, C, own, 2 * each, endpoints)
    part_hist = full.reshape(GROUPS, C, nblk, 2, LANES).transpose(0, 1, 3, 2, 4).reshape(GROUPS, C, 2, bins)
    part_tns = part_tns.transpose(2, 0, 1)
    part_share = part_share.reshape(GROUPS)
    return (part_hist, part_tns, part_share, tns, wns, worst)


def solution(mesh):
    in_specs = (
        P("corner", "ep"),
        P("corner", "ep"),
        P("corner", "ep"),
        P("corner", "ep"),
        P("ep"),
        P(),
    )
    out_specs = (
        P(None, "corner", None, None),
        P(None, "corner", None),
        P(),
        P("corner", None),
        P("corner", None),
        P(None, "ep"),
    )
    return jax.shard_map(
        on_device, mesh=mesh, in_specs=in_specs, out_specs=out_specs, check_vma=False
    )
```

```python
import functools
import jax
import jax.numpy as jnp
from jax import lax
from jax.experimental import pallas as pl
from jax.experimental.pallas import tpu as pltpu
from jax.sharding import PartitionSpec as P

GROUPS = 64
LANES = 128
LEAST = 4096
F8 = jnp.float8_e4m3fn
BF = jnp.bfloat16
STEP = 0.001
VMEM = 12 << 20
EXTRA = 8


def lookup(table_ref, index):
    lane = index & (LANES - 1)
    row = index >> 7
    out = None
    for r in range(table_ref.shape[0]):
        line = jnp.broadcast_to(table_ref[r:r + 1, :], index.shape)
        got = jnp.take_along_axis(line, lane, axis=1, mode="promise_in_bounds")
        out = got if out is None else jnp.where(row == r, got, out)
    return out


def interval(slack, x0, coarse_ref, fine_ref):
    t = jnp.minimum(jnp.maximum(slack, x0), 0.0)
    whole = jnp.floor(t * 1000.0)
    whole = jnp.where(t >= (whole + 1.0) * jnp.float32(STEP), whole + 1.0, whole)
    whole = jnp.where(t < whole * jnp.float32(STEP), whole - 1.0, whole)
    q = jnp.minimum(whole.astype(jnp.int32) + LEAST, LEAST - 1)
    cell = lookup(coarse_ref, q >> 3)
    upto = jnp.left_shift(2, q & 7) - 1
    j = (cell & 0xFFFF) + lax.population_count((cell >> 16) & upto) - 1
    pair = lookup(fine_ref, j)
    k = (pair & 0xFFFF) - LEAST
    x = k.astype(jnp.float32) * jnp.float32(STEP)
    xn = (k + (pair >> 16)).astype(jnp.float32) * jnp.float32(STEP)
    r = 1.0 / (xn - x)
    w1 = jnp.maximum((xn - t) * r, 0.0)
    w2 = jnp.maximum((t - x) * r, 0.0)
    local = j & (LANES - 1)
    odd = (j & 1) == 1
    even_place = ((local + 1) & ~1).astype(jnp.float32)
    odd_place = (local | 1).astype(jnp.float32)
    return (
        even_place,
        odd_place,
        jnp.where(odd, w2, w1),
        jnp.where(odd, w1, w2),
        (j >> 7).astype(jnp.float32),
        jnp.minimum(slack, 0.0),
    )


def prep_kernel(
    C, edges_ref, side_ref, lines_ref, *refs
):
    sources, refs = refs[:5], refs[5:]
    (coarse_ref, fine_ref, worst_ref, keep_ref, send_ref), held, sems = refs[:5], refs[5:10], refs[10]
    copies = [pltpu.make_async_copy(src, dst, sems.at[i]) for i, (src, dst) in enumerate(zip(sources, held))]
    for copy in copies:
        copy.start()
    ids_ref, a_ref, b_ref, c_ref, d_ref = held
    bins = edges_ref.shape[0]
    cell = lax.broadcasted_iota(jnp.int32, coarse_ref.shape, 0) * LANES + lax.broadcasted_iota(
        jnp.int32, coarse_ref.shape, 1
    )
    zero = jnp.zeros(coarse_ref.shape, jnp.int32)

    def add(i, state):
        state = list(state)
        for u in range(16):
            q = edges_ref[i * 16 + u] + LEAST
            here = q >> 3
            base, bits = state[u % 4]
            base = base + jnp.where(cell > here, 1, 0)
            bits = bits + jnp.where(cell == here, jnp.left_shift(65536, q & 7), 0)
            state[u % 4] = (base, bits)
        return tuple(state)

    state = lax.fori_loop(0, bins // 16, add, tuple((zero, zero) for _ in range(4)))
    coarse_ref[...] = sum(base + bits for base, bits in state)
    q = lines_ref[...] + LEAST
    _, lanes = q.shape
    left = pltpu.roll(q, lanes - 1, 1)
    below = jnp.concatenate([left[1:], jnp.full((1, lanes), LEAST, jnp.int32)], axis=0)
    last = lax.broadcasted_iota(jnp.int32, q.shape, 1) == lanes - 1
    following = jnp.where(last, below, left)
    fine_ref[...] = q + (following - q) * 65536

    for copy in copies:
        copy.wait()
    flag = side_ref[0] == 0
    half = C // 2
    lines = a_ref.shape[0] // C
    for m, (late, early) in enumerate(((a_ref, b_ref), (c_ref, d_ref))):
        for k in range(half):
            pieces = []
            for c in (k, k + half):
                at = pl.ds(c, lines, stride=C)
                pieces.append(late[at, :] - early[at, :])
            keep_ref[m, pl.ds(k, lines, stride=half), :] = jnp.where(flag, pieces[0], pieces[1])
            send_ref[m, pl.ds(k, lines, stride=half), :] = jnp.where(flag, pieces[1], pieces[0])
            for piece in pieces:
                first = k == 0 and piece is pieces[0]
                at = pl.ds(m, lines, stride=2)
                worst_ref[at, :] = piece if first else jnp.minimum(worst_ref[at, :], piece)
    ids = ids_ref[...].astype(jnp.float32)
    keep_ref[2, :lines, :] = ids
    send_ref[2, :lines, :] = ids


def run_prep(edges, side, ids, a, b, c, d, C):
    bins = edges.shape[0]
    lines = ids.shape[0]
    smem = pl.BlockSpec(memory_space=pltpu.SMEM)
    return pl.pallas_call(
        functools.partial(prep_kernel, C),
        in_specs=[smem, smem, pl.BlockSpec(memory_space=pltpu.VMEM)] + [pl.BlockSpec(memory_space=pltpu.HBM)] * 5,
        out_shape=[
            jax.ShapeDtypeStruct((LEAST // 8 // LANES, LANES), jnp.int32),
            jax.ShapeDtypeStruct((bins // LANES, LANES), jnp.int32),
            jax.ShapeDtypeStruct((2 * lines, LANES), jnp.float32),
            jax.ShapeDtypeStruct((3, lines * C // 2, LANES), jnp.float32),
            jax.ShapeDtypeStruct((3, lines * C // 2, LANES), jnp.float32),
        ],
        scratch_shapes=[pltpu.VMEM(x.shape, x.dtype) for x in (ids, a, b, c, d)] + [pltpu.SemaphoreType.DMA((5,))],
        compiler_params=pltpu.CompilerParams(vmem_limit_bytes=VMEM),
        name="prep",
    )(edges, side, pltpu.with_memory_space_constraint(edges.reshape(-1, LANES), pltpu.HBM), ids, a, b, c, d)


def hist_kernel(C, KT, n, edges_ref, place_ref, coarse_ref, fine_ref, slack_ref, *refs):
    if n:
        prior_ref, prior_low_ref = refs[:2]
        outs, (low_ref, buf0, buf1, all_ref) = refs[2:2 + n], refs[2 + n:]
    else:
        out_ref, low_ref, buf0, buf1 = refs
    series = 2 * C
    nblk = fine_ref.shape[0]
    lines = KT * C
    chunks = slack_ref.shape[1] // lines
    x0 = edges_ref[0].astype(jnp.float32) * jnp.float32(STEP)

    def body(*accs):
        for a in accs:
            pltpu.matmul_pop(a)
        iota16 = lax.broadcasted_iota(jnp.int32, (16, LANES), 0)
        iotas = [(iota16 + 16 * v).astype(jnp.float32).astype(BF) for v in range(LANES // 16)]
        iota32 = lax.broadcasted_iota(jnp.int32, (32, LANES), 0)
        iotas32 = [(iota32 + 32 * v).astype(jnp.float32).astype(BF) for v in range(GROUPS // 32)]
        even = (iota16 & 1) == 0
        iota8 = lax.broadcasted_iota(jnp.int32, (8, LANES), 0)
        one = jnp.ones((32, LANES), BF)
        zero16 = jnp.zeros((16, LANES), BF)
        zero32 = jnp.zeros((32, LANES), BF)
        none = jnp.zeros((32, LANES), F8)
        tail = jnp.where(iota8 == 3, 1.0, 0.0)

        def wide(x, rows):
            return jnp.broadcast_to(x, (rows, LANES))

        def look(buf, chunk, g):
            start = pl.multiple_of(chunk * lines + g * 8, 8)
            at = pl.ds(start, 8)
            for m in range(2):
                slack = slack_ref[m, at, :]
                low_ref[m] = jnp.minimum(low_ref[m], slack)
                for i, v in enumerate(interval(slack, x0, coarse_ref, fine_ref)):
                    buf[i, m, g * 8:g * 8 + 8, :] = v

        def pair(buf, chunk, k2):
            member = []
            for kk in range(2):
                ids = wide(slack_ref[2, pl.ds(chunk * KT + 2 * k2 + kk, 1), :], 32).astype(BF)
                member.append([jnp.where(i == ids, one, zero32).astype(F8) for i in iotas32])
            for s in range(series):
                c, m = divmod(s, 2)
                left, right = [], []
                for kk in range(2):
                    r = (2 * k2 + kk) * C + c
                    row = [buf[i, m, r:r + 1, :] for i in range(6)]
                    block = wide(row[4], 32).astype(BF)
                    left.append(jnp.concatenate([
                        jnp.where(block == jnp.bfloat16(h), part, none) for h in range(nblk) for part in member[kk]
                    ], axis=0))
                    place = jnp.where(even, wide(row[0], 16), wide(row[1], 16)).astype(BF)
                    weight = jnp.where(even, wide(row[2], 16), wide(row[3], 16)).astype(BF)
                    hats = [jnp.where(i == place, weight, zero16) for i in iotas]
                    negative = wide(row[5], 8)
                    high = negative.astype(BF).astype(jnp.float32)
                    cross = jnp.where(wide(row[0], 8) == float(LANES), wide(row[2], 8), 0.0)
                    z = jnp.where(iota8 == 2, cross, tail)
                    z = jnp.where(iota8 == 0, high, jnp.where(iota8 == 1, negative - high, z))
                    hats.append(jnp.concatenate([z, jnp.zeros((8, LANES), jnp.float32)], axis=0).astype(BF))
                    right.append(jnp.concatenate(hats, axis=0))
                pltpu.matmul_push_rhs(
                    jnp.concatenate(left, axis=1), staging_register=0, mxu_index=s % 2, transpose=True
                )
                pltpu.matmul_acc_lhs(accs[s], jnp.concatenate(right, axis=1), load_staged_rhs=0)

        def both(chunk, buf, ahead, other):
            pairs, groups = KT // 2, lines // 8
            done = 0
            for k2 in range(pairs):
                pair(buf, chunk, k2)
                while done < groups and done * pairs <= k2 * groups:
                    look(other, ahead, done)
                    done += 1

        low_ref[...] = prior_low_ref[...] if n else jnp.full(low_ref.shape, jnp.inf)
        for g in range(lines // 8):
            look(buf0, 0, g)

        def two(i, carry):
            both(2 * i, buf0, 2 * i + 1, buf1)
            both(2 * i + 1, buf1, jnp.minimum(2 * i + 2, chunks - 1), buf0)
            return carry

        lax.fori_loop(0, chunks // 2, two, 0)

        sums = [pltpu.matmul_pop(a) for a in accs]
        if not n:
            for s in range(series):
                out_ref[s] = sums[s]
            return
        own = GROUPS // n
        lane = lax.broadcasted_iota(jnp.int32, (8, LANES), 1)
        sub = lax.broadcasted_iota(jnp.int32, (8, LANES), 0)
        wide_lane = lax.broadcasted_iota(jnp.int32, (8, nblk * GROUPS), 1)
        wide_sub = lax.broadcasted_iota(jnp.int32, (8, nblk * GROUPS), 0)
        chunk_rows = outs[0].shape[0]
        hist_rows = own * series * nblk
        tile = jnp.zeros((8, LANES), jnp.float32)
        for s in range(series):
            c, m = divmod(s, 2)
            total = prior_ref[s] + sums[s]
            stats = total[LANES:LANES + 8]
            across = jnp.broadcast_to(pltpu.roll(stats, GROUPS, 1)[2:3], wide_lane.shape)
            top = total[:8] + jnp.where((wide_sub == 0) & (wide_lane >= GROUPS), across, 0.0)
            full = jnp.concatenate([top, total[8:LANES]], axis=0).T
            folded = stats[:, :LANES]
            for v in range(1, nblk * GROUPS // LANES):
                folded = folded + stats[:, v * LANES:(v + 1) * LANES]
            folded = folded + pltpu.roll(folded, GROUPS, 1)
            low = jnp.min(jnp.where(sub % C == c, low_ref[m], jnp.inf), keepdims=True)
            row = jnp.where(lane < GROUPS, folded[0:1] + folded[1:2], low)
            tile = jnp.where(sub == s, row, tile)
            if s == 0:
                tile = jnp.where(sub == series, folded[3:4], tile)
            for h in range(nblk):
                for i in range(n):
                    at = i * chunk_rows + (c * nblk + h) * 2 + m
                    first = h * GROUPS + i * own
                    all_ref[pl.ds(at, own, stride=series * nblk), :] = full[first:first + own]
        for i in range(n):
            at = i * chunk_rows + hist_rows
            all_ref[at:at + EXTRA, :] = tile
        for d in range(n):
            at = pl.multiple_of(lax.rem(place_ref[0] + d, n) * chunk_rows, 8)
            outs[d][...] = all_ref[pl.ds(at, chunk_rows), :]

    pl.run_scoped(body, *[pltpu.ACC(s % 2)((LANES + 16, 256), jnp.float32) for s in range(series)])


def run_hist(edges, place, coarse, fine, slack, C, n=0, prior=(), KT=16):
    nblk = fine.shape[0]
    series = 2 * C
    smem = pl.BlockSpec(memory_space=pltpu.SMEM)
    vm = pl.BlockSpec(memory_space=pltpu.VMEM)
    scratch = [pltpu.VMEM((6, 2, KT * C, LANES), jnp.float32) for _ in range(2)]
    low = jax.ShapeDtypeStruct((2, 8, LANES), jnp.float32)
    if n:
        own = GROUPS // n
        rows = own * series * nblk + EXTRA
        outs = [jax.ShapeDtypeStruct((rows, LANES), jnp.float32) for _ in range(n)]
        scratch += [pltpu.VMEM((2, 8, LANES), jnp.float32)] * 0 + [pltpu.VMEM((n * rows, LANES), jnp.float32)]
    else:
        outs = [jax.ShapeDtypeStruct((series, LANES + 16, nblk * GROUPS), jnp.float32)]
    return pl.pallas_call(
        functools.partial(hist_kernel, C, KT, n),
        in_specs=[smem, smem] + [vm] * (3 + len(prior)),
        out_shape=outs + [low],
        scratch_shapes=scratch,
        cost_estimate=pl.CostEstimate(
            flops=4 * (LANES + 16) * 256 * slack.size // 3, bytes_accessed=8 * slack.size, transcendentals=slack.size
        ),
        compiler_params=pltpu.CompilerParams(vmem_limit_bytes=VMEM),
        name="hist",
    )(edges, place, coarse, fine, slack, *prior)


def final_kernel(C, own, share, scale, me_ref, *refs):
    n = len(refs) - 5
    pieces = refs[:n]
    hist_ref, part_ref, share_ref, tns_ref, wns_ref = refs[n:]
    half = C // 2
    each = hist_ref.shape[0] // GROUPS // 2
    for d in range(n):
        source = lax.rem(me_ref[0] - d + n, n)
        place, side = source >> 1, source & 1
        for p in range(own):
            at = pl.multiple_of((place * own + p) * 2 * each + side * each, 8)
            hist_ref[pl.ds(at, each), :] = pieces[d][p * each:(p + 1) * each, :]
    tns = jnp.zeros((C, 2), jnp.float32)
    wns = jnp.zeros((C, 2), jnp.float32)
    row = lax.broadcasted_iota(jnp.int32, (C, 2), 0)
    col = lax.broadcasted_iota(jnp.int32, (C, 2), 1)
    mine, other = pieces[0][own * each:, :], pieces[1][own * each:, :]
    even = me_ref[0] % 2 == 0
    for side in range(2):
        tile = jnp.where(even, mine, other) if side == 0 else jnp.where(even, other, mine)
        for s in range(2 * half):
            c, m = divmod(s, 2)
            c += side * half
            sums = tile[s:s + 1, :GROUPS]
            part_ref[c, m:m + 1, :] = sums * share
            here = (row == c) & (col == m)
            tns = jnp.where(here, jnp.sum(sums, keepdims=True) * scale, tns)
            wns = jnp.where(here, tile[s:s + 1, GROUPS:GROUPS + 1], wns)
    share_ref[...] = mine[2 * half:2 * half + 1, :GROUPS] * share
    tns_ref[...] = tns
    wns_ref[...] = wns


def run_final(me, pieces, C, own, rows, endpoints):
    vm = pl.BlockSpec(memory_space=pltpu.VMEM)
    return pl.pallas_call(
        functools.partial(final_kernel, C, own, GROUPS / endpoints, 1.0 / endpoints),
        in_specs=[pl.BlockSpec(memory_space=pltpu.SMEM)] + [vm] * len(pieces),
        out_shape=[
            jax.ShapeDtypeStruct((GROUPS * rows, LANES), jnp.float32),
            jax.ShapeDtypeStruct((C, 2, GROUPS), jnp.float32),
            jax.ShapeDtypeStruct((1, GROUPS), jnp.float32),
            jax.ShapeDtypeStruct((C, 2), jnp.float32),
            jax.ShapeDtypeStruct((C, 2), jnp.float32),
        ],
        compiler_params=pltpu.CompilerParams(vmem_limit_bytes=VMEM),
        name="final",
    )(me, *pieces)


def rotate(value, axis, distance):
    size = lax.axis_size(axis)
    return lax.ppermute(value, axis, [(i, (i + distance) % size) for i in range(size)])


def tiles(x):
    c, e = x.shape
    return x.reshape(c, e // LANES, LANES).transpose(1, 0, 2).reshape(-1, LANES)


def on_device(required, arrival, hold_required, early_arrival, part_ids, bin_edges):
    C, rows = required.shape
    bins = bin_edges.shape[0]
    n = lax.axis_size("ep")
    me = lax.axis_index("ep")
    endpoints = rows * n
    density = GROUPS * bins / endpoints
    half = C // 2
    side = me % 2
    place = me // 2
    rest = n // 2
    data = (tiles(required), tiles(arrival), tiles(early_arrival), tiles(hold_required))
    ids = part_ids.reshape(-1, LANES)
    data = tuple(pltpu.with_memory_space_constraint(x, pltpu.HBM) for x in data)
    lines = ids.shape[0]
    coarse, fine, near, keep, send = run_prep(bin_edges, side.reshape(1), pltpu.with_memory_space_constraint(ids, pltpu.HBM), *data, C)
    got = lax.ppermute(send, "ep", [(i, i ^ 1) for i in range(n)])
    shares = [rotate(near, "corner", d) for d in range(1, lax.axis_size("corner"))]
    prior = run_hist(bin_edges, place.reshape(1), coarse, fine, keep, half)
    chunks = run_hist(bin_edges, place.reshape(1), coarse, fine, got, half, rest, prior)
    worst = functools.reduce(jnp.minimum, shares, near).reshape(lines, 2, LANES)
    worst = worst.transpose(1, 0, 2).reshape(2, rows)

    own = GROUPS // rest
    nblk = bins // LANES
    each = C * nblk
    hrows = own * each
    total = chunks[0]
    row = lax.broadcasted_iota(jnp.int32, total.shape, 0)
    lane = lax.broadcasted_iota(jnp.int32, total.shape, 1)
    least = (row >= hrows) & (row < hrows + 2 * half) & (lane >= GROUPS)
    for d in range(1, rest):
        piece = rotate(chunks[d], "ep", 2 * d)
        total = jnp.where(least, jnp.minimum(total, piece), total + piece)
    mine = jnp.where(row < hrows, total * density, total)
    pieces = [rotate(mine, "ep", d) if d else mine for d in range(n)]
    full, part_tns, part_share, tns, wns = run_final(me.reshape(1), pieces, C, own, 2 * each, endpoints)
    part_hist = full.reshape(GROUPS, C, nblk, 2, LANES).transpose(0, 1, 3, 2, 4).reshape(GROUPS, C, 2, bins)
    part_tns = part_tns.transpose(2, 0, 1)
    part_share = part_share.reshape(GROUPS)
    return (part_hist, part_tns, part_share, tns, wns, worst)


def solution(mesh):
    in_specs = (
        P("corner", "ep"),
        P("corner", "ep"),
        P("corner", "ep"),
        P("corner", "ep"),
        P("ep"),
        P(),
    )
    out_specs = (
        P(None, "corner", None, None),
        P(None, "corner", None),
        P(),
        P("corner", None),
        P("corner", None),
        P(None, "ep"),
    )
    return jax.shard_map(
        on_device, mesh=mesh, in_specs=in_specs, out_specs=out_specs, check_vma=False
    )
```

```python
import functools
import jax
import jax.numpy as jnp
from jax import lax
from jax.experimental import pallas as pl
from jax.experimental.pallas import tpu as pltpu
from jax.sharding import PartitionSpec as P

GROUPS = 64
LANES = 128
LEAST = 4096
F8 = jnp.float8_e4m3fn
BF = jnp.bfloat16
STEP = 0.001
VMEM = 12 << 20
EXTRA = 8


def lookup(table_ref, index):
    lane = index & (LANES - 1)
    row = index >> 7
    out = None
    for r in range(table_ref.shape[0]):
        line = jnp.broadcast_to(table_ref[r:r + 1, :], index.shape)
        got = jnp.take_along_axis(line, lane, axis=1, mode="promise_in_bounds")
        out = got if out is None else jnp.where(row == r, got, out)
    return out


def interval(slack, x0, coarse_ref, fine_ref):
    t = jnp.minimum(jnp.maximum(slack, x0), 0.0)
    whole = jnp.floor(t * 1000.0)
    whole = jnp.where(t >= (whole + 1.0) * jnp.float32(STEP), whole + 1.0, whole)
    whole = jnp.where(t < whole * jnp.float32(STEP), whole - 1.0, whole)
    q = jnp.minimum(whole.astype(jnp.int32) + LEAST, LEAST - 1)
    cell = lookup(coarse_ref, q >> 3)
    upto = jnp.left_shift(2, q & 7) - 1
    j = (cell & 0xFFFF) + lax.population_count((cell >> 16) & upto) - 1
    pair = lookup(fine_ref, j)
    k = (pair & 0xFFFF) - LEAST
    x = k.astype(jnp.float32) * jnp.float32(STEP)
    xn = (k + (pair >> 16)).astype(jnp.float32) * jnp.float32(STEP)
    r = 1.0 / (xn - x)
    w1 = jnp.maximum((xn - t) * r, 0.0)
    w2 = jnp.maximum((t - x) * r, 0.0)
    local = j & (LANES - 1)
    odd = (j & 1) == 1
    even_place = ((local + 1) & ~1).astype(jnp.float32)
    odd_place = (local | 1).astype(jnp.float32)
    return (
        even_place,
        odd_place,
        jnp.where(odd, w2, w1),
        jnp.where(odd, w1, w2),
        (j >> 7).astype(jnp.float32),
        jnp.minimum(slack, 0.0),
    )


def prep_kernel(C, side_ref, *refs):
    sources, refs = refs[:7], refs[7:]
    (coarse_ref, fine_ref, worst_ref, keep_ref, send_ref), held, sems = refs[:5], refs[5:12], refs[12]
    copies = [pltpu.make_async_copy(src, dst, sems.at[i]) for i, (src, dst) in enumerate(zip(sources, held))]
    for copy in copies:
        copy.start()
    edges_ref, lines_ref, ids_ref, a_ref, b_ref, c_ref, d_ref = held
    copies[0].wait()
    copies[1].wait()
    bins = edges_ref.shape[0]
    cell = lax.broadcasted_iota(jnp.int32, coarse_ref.shape, 0) * LANES + lax.broadcasted_iota(
        jnp.int32, coarse_ref.shape, 1
    )
    zero = jnp.zeros(coarse_ref.shape, jnp.int32)

    def add(i, state):
        state = list(state)
        for u in range(16):
            q = edges_ref[i * 16 + u] + LEAST
            here = q >> 3
            base, bits = state[u % 4]
            base = base + jnp.where(cell > here, 1, 0)
            bits = bits + jnp.where(cell == here, jnp.left_shift(65536, q & 7), 0)
            state[u % 4] = (base, bits)
        return tuple(state)

    state = lax.fori_loop(0, bins // 16, add, tuple((zero, zero) for _ in range(4)))
    coarse_ref[...] = sum(base + bits for base, bits in state)
    q = lines_ref[...] + LEAST
    _, lanes = q.shape
    left = pltpu.roll(q, lanes - 1, 1)
    below = jnp.concatenate([left[1:], jnp.full((1, lanes), LEAST, jnp.int32)], axis=0)
    last = lax.broadcasted_iota(jnp.int32, q.shape, 1) == lanes - 1
    following = jnp.where(last, below, left)
    fine_ref[...] = q + (following - q) * 65536

    for copy in copies[2:]:
        copy.wait()
    flag = side_ref[0] == 0
    half = C // 2
    lines = a_ref.shape[0] // C
    for m, (late, early) in enumerate(((a_ref, b_ref), (c_ref, d_ref))):
        for k in range(half):
            pieces = []
            for c in (k, k + half):
                at = pl.ds(c, lines, stride=C)
                pieces.append(late[at, :] - early[at, :])
            keep_ref[m, pl.ds(k, lines, stride=half), :] = jnp.where(flag, pieces[0], pieces[1])
            send_ref[m, pl.ds(k, lines, stride=half), :] = jnp.where(flag, pieces[1], pieces[0])
            for piece in pieces:
                first = k == 0 and piece is pieces[0]
                at = pl.ds(m, lines, stride=2)
                worst_ref[at, :] = piece if first else jnp.minimum(worst_ref[at, :], piece)
    ids = ids_ref[...].astype(jnp.float32)
    keep_ref[2, :lines, :] = ids
    send_ref[2, :lines, :] = ids


def run_prep(edges, side, ids, a, b, c, d, C):
    bins = edges.shape[0]
    lines = ids.shape[0]
    sources = (edges, edges.reshape(-1, LANES), ids, a, b, c, d)
    sources = [pltpu.with_memory_space_constraint(x, pltpu.HBM) for x in sources]
    held = [pltpu.SMEM(edges.shape, edges.dtype)] + [pltpu.VMEM(x.shape, x.dtype) for x in sources[1:]]
    return pl.pallas_call(
        functools.partial(prep_kernel, C),
        in_specs=[pl.BlockSpec(memory_space=pltpu.SMEM)] + [pl.BlockSpec(memory_space=pltpu.HBM)] * 7,
        out_shape=[
            jax.ShapeDtypeStruct((LEAST // 8 // LANES, LANES), jnp.int32),
            jax.ShapeDtypeStruct((bins // LANES, LANES), jnp.int32),
            jax.ShapeDtypeStruct((2 * lines, LANES), jnp.float32),
            jax.ShapeDtypeStruct((3, lines * C // 2, LANES), jnp.float32),
            jax.ShapeDtypeStruct((3, lines * C // 2, LANES), jnp.float32),
        ],
        scratch_shapes=held + [pltpu.SemaphoreType.DMA((7,))],
        compiler_params=pltpu.CompilerParams(vmem_limit_bytes=VMEM),
        name="prep",
    )(side, *sources)


def hist_kernel(C, KT, n, place_ref, coarse_ref, fine_ref, slack_ref, *refs):
    if n:
        prior_ref, prior_low_ref = refs[:2]
        outs, (low_ref, buf0, buf1, all_ref) = refs[2:2 + n], refs[2 + n:]
    else:
        out_ref, low_ref, buf0, buf1 = refs
    series = 2 * C
    nblk = fine_ref.shape[0]
    lines = KT * C
    chunks = slack_ref.shape[1] // lines
    x0 = ((fine_ref[:1, :1] & 0xFFFF) - LEAST).astype(jnp.float32) * jnp.float32(STEP)

    def body(*accs):
        for a in accs:
            pltpu.matmul_pop(a)
        iota16 = lax.broadcasted_iota(jnp.int32, (16, LANES), 0)
        iotas = [(iota16 + 16 * v).astype(jnp.float32).astype(BF) for v in range(LANES // 16)]
        iota32 = lax.broadcasted_iota(jnp.int32, (32, LANES), 0)
        iotas32 = [(iota32 + 32 * v).astype(jnp.float32).astype(BF) for v in range(GROUPS // 32)]
        even = (iota16 & 1) == 0
        iota8 = lax.broadcasted_iota(jnp.int32, (8, LANES), 0)
        one = jnp.ones((32, LANES), BF)
        zero16 = jnp.zeros((16, LANES), BF)
        zero32 = jnp.zeros((32, LANES), BF)
        none = jnp.zeros((32, LANES), F8)
        tail = jnp.where(iota8 == 3, 1.0, 0.0)

        def wide(x, rows):
            return jnp.broadcast_to(x, (rows, LANES))

        def look(buf, chunk, g):
            start = pl.multiple_of(chunk * lines + g * 8, 8)
            at = pl.ds(start, 8)
            for m in range(2):
                slack = slack_ref[m, at, :]
                low_ref[m] = jnp.minimum(low_ref[m], slack)
                for i, v in enumerate(interval(slack, x0, coarse_ref, fine_ref)):
                    buf[i, m, g * 8:g * 8 + 8, :] = v

        def pair(buf, chunk, k2):
            member = []
            for kk in range(2):
                ids = wide(slack_ref[2, pl.ds(chunk * KT + 2 * k2 + kk, 1), :], 32).astype(BF)
                member.append([jnp.where(i == ids, one, zero32).astype(F8) for i in iotas32])
            for s in range(series):
                c, m = divmod(s, 2)
                left, right = [], []
                for kk in range(2):
                    r = (2 * k2 + kk) * C + c
                    row = [buf[i, m, r:r + 1, :] for i in range(6)]
                    block = wide(row[4], 32).astype(BF)
                    left.append(jnp.concatenate([
                        jnp.where(block == jnp.bfloat16(h), part, none) for h in range(nblk) for part in member[kk]
                    ], axis=0))
                    place = jnp.where(even, wide(row[0], 16), wide(row[1], 16)).astype(BF)
                    weight = jnp.where(even, wide(row[2], 16), wide(row[3], 16)).astype(BF)
                    hats = [jnp.where(i == place, weight, zero16) for i in iotas]
                    negative = wide(row[5], 8)
                    high = negative.astype(BF).astype(jnp.float32)
                    cross = jnp.where(wide(row[0], 8) == float(LANES), wide(row[2], 8), 0.0)
                    z = jnp.where(iota8 == 2, cross, tail)
                    z = jnp.where(iota8 == 0, high, jnp.where(iota8 == 1, negative - high, z))
                    hats.append(jnp.concatenate([z, jnp.zeros((8, LANES), jnp.float32)], axis=0).astype(BF))
                    right.append(jnp.concatenate(hats, axis=0))
                pltpu.matmul_push_rhs(
                    jnp.concatenate(left, axis=1), staging_register=0, mxu_index=s % 2, transpose=True
                )
                pltpu.matmul_acc_lhs(accs[s], jnp.concatenate(right, axis=1), load_staged_rhs=0)

        def both(chunk, buf, ahead, other):
            pairs, groups = KT // 2, lines // 8
            done = 0
            for k2 in range(pairs):
                pair(buf, chunk, k2)
                while done < groups and done * pairs <= k2 * groups:
                    look(other, ahead, done)
                    done += 1

        low_ref[...] = prior_low_ref[...] if n else jnp.full(low_ref.shape, jnp.inf)
        for g in range(lines // 8):
            look(buf0, 0, g)

        def two(i, carry):
            both(2 * i, buf0, 2 * i + 1, buf1)
            both(2 * i + 1, buf1, jnp.minimum(2 * i + 2, chunks - 1), buf0)
            return carry

        lax.fori_loop(0, chunks // 2, two, 0)

        sums = [pltpu.matmul_pop(a) for a in accs]
        if not n:
            for s in range(series):
                out_ref[s] = sums[s]
            return
        own = GROUPS // n
        lane = lax.broadcasted_iota(jnp.int32, (8, LANES), 1)
        sub = lax.broadcasted_iota(jnp.int32, (8, LANES), 0)
        wide_lane = lax.broadcasted_iota(jnp.int32, (8, nblk * GROUPS), 1)
        wide_sub = lax.broadcasted_iota(jnp.int32, (8, nblk * GROUPS), 0)
        chunk_rows = outs[0].shape[0]
        hist_rows = own * series * nblk
        tile = jnp.zeros((8, LANES), jnp.float32)
        for s in range(series):
            c, m = divmod(s, 2)
            total = prior_ref[s] + sums[s]
            stats = total[LANES:LANES + 8]
            across = jnp.broadcast_to(pltpu.roll(stats, GROUPS, 1)[2:3], wide_lane.shape)
            top = total[:8] + jnp.where((wide_sub == 0) & (wide_lane >= GROUPS), across, 0.0)
            full = jnp.concatenate([top, total[8:LANES]], axis=0).T
            folded = stats[:, :LANES]
            for v in range(1, nblk * GROUPS // LANES):
                folded = folded + stats[:, v * LANES:(v + 1) * LANES]
            folded = folded + pltpu.roll(folded, GROUPS, 1)
            low = jnp.min(jnp.where(sub % C == c, low_ref[m], jnp.inf), keepdims=True)
            row = jnp.where(lane < GROUPS, folded[0:1] + folded[1:2], low)
            tile = jnp.where(sub == s, row, tile)
            if s == 0:
                tile = jnp.where(sub == series, folded[3:4], tile)
            for h in range(nblk):
                for i in range(n):
                    at = i * chunk_rows + (c * nblk + h) * 2 + m
                    first = h * GROUPS + i * own
                    all_ref[pl.ds(at, own, stride=series * nblk), :] = full[first:first + own]
        for i in range(n):
            at = i * chunk_rows + hist_rows
            all_ref[at:at + EXTRA, :] = tile
        for d in range(n):
            at = pl.multiple_of((place_ref[0] ^ d) * chunk_rows, 8)
            outs[d][...] = all_ref[pl.ds(at, chunk_rows), :]

    pl.run_scoped(body, *[pltpu.ACC(s % 2)((LANES + 16, 256), jnp.float32) for s in range(series)])


def run_hist(place, coarse, fine, slack, C, n=0, prior=(), KT=16):
    nblk = fine.shape[0]
    series = 2 * C
    smem = pl.BlockSpec(memory_space=pltpu.SMEM)
    vm = pl.BlockSpec(memory_space=pltpu.VMEM)
    scratch = [pltpu.VMEM((6, 2, KT * C, LANES), jnp.float32) for _ in range(2)]
    low = jax.ShapeDtypeStruct((2, 8, LANES), jnp.float32)
    if n:
        own = GROUPS // n
        rows = own * series * nblk + EXTRA
        outs = [jax.ShapeDtypeStruct((rows, LANES), jnp.float32) for _ in range(n)]
        scratch += [pltpu.VMEM((2, 8, LANES), jnp.float32)] * 0 + [pltpu.VMEM((n * rows, LANES), jnp.float32)]
    else:
        outs = [jax.ShapeDtypeStruct((series, LANES + 16, nblk * GROUPS), jnp.float32)]
    return pl.pallas_call(
        functools.partial(hist_kernel, C, KT, n),
        in_specs=[smem] + [vm] * (3 + len(prior)),
        out_shape=outs + [low],
        scratch_shapes=scratch,
        cost_estimate=pl.CostEstimate(
            flops=4 * (LANES + 16) * 256 * slack.size // 3, bytes_accessed=8 * slack.size, transcendentals=slack.size
        ),
        compiler_params=pltpu.CompilerParams(vmem_limit_bytes=VMEM),
        name="hist",
    )(place, coarse, fine, slack, *prior)


def final_kernel(C, own, share, scale, me_ref, *refs):
    n = len(refs) - 5
    pieces = refs[:n]
    hist_ref, part_ref, share_ref, tns_ref, wns_ref = refs[n:]
    half = C // 2
    each = hist_ref.shape[0] // GROUPS // 2
    for d in range(n):
        source = me_ref[0] ^ d
        place, side = source >> 1, source & 1
        for p in range(own):
            at = pl.multiple_of((place * own + p) * 2 * each + side * each, 8)
            hist_ref[pl.ds(at, each), :] = pieces[d][p * each:(p + 1) * each, :]
    tns = jnp.zeros((C, 2), jnp.float32)
    wns = jnp.zeros((C, 2), jnp.float32)
    row = lax.broadcasted_iota(jnp.int32, (C, 2), 0)
    col = lax.broadcasted_iota(jnp.int32, (C, 2), 1)
    mine, other = pieces[0][own * each:, :], pieces[1][own * each:, :]
    even = me_ref[0] % 2 == 0
    for side in range(2):
        tile = jnp.where(even, mine, other) if side == 0 else jnp.where(even, other, mine)
        for s in range(2 * half):
            c, m = divmod(s, 2)
            c += side * half
            sums = tile[s:s + 1, :GROUPS]
            part_ref[c, m:m + 1, :] = sums * share
            here = (row == c) & (col == m)
            tns = jnp.where(here, jnp.sum(sums, keepdims=True) * scale, tns)
            wns = jnp.where(here, tile[s:s + 1, GROUPS:GROUPS + 1], wns)
    share_ref[...] = mine[2 * half:2 * half + 1, :GROUPS] * share
    tns_ref[...] = tns
    wns_ref[...] = wns


def run_final(me, pieces, C, own, rows, endpoints):
    vm = pl.BlockSpec(memory_space=pltpu.VMEM)
    return pl.pallas_call(
        functools.partial(final_kernel, C, own, GROUPS / endpoints, 1.0 / endpoints),
        in_specs=[pl.BlockSpec(memory_space=pltpu.SMEM)] + [vm] * len(pieces),
        out_shape=[
            jax.ShapeDtypeStruct((GROUPS * rows, LANES), jnp.float32),
            jax.ShapeDtypeStruct((C, 2, GROUPS), jnp.float32),
            jax.ShapeDtypeStruct((1, GROUPS), jnp.float32),
            jax.ShapeDtypeStruct((C, 2), jnp.float32),
            jax.ShapeDtypeStruct((C, 2), jnp.float32),
        ],
        compiler_params=pltpu.CompilerParams(vmem_limit_bytes=VMEM),
        name="final",
    )(me, *pieces)


def rotate(value, axis, distance):
    size = lax.axis_size(axis)
    return lax.ppermute(value, axis, [(i, (i + distance) % size) for i in range(size)])


def turned(index, odd):
    return jnp.where(odd, (index & ~3) | ((index & 1) << 1) | ((index >> 1) & 1), index)


def moved(value, target):
    n, blocks = lax.axis_size("ep"), lax.axis_size("corner")

    def place(i, k):
        return (i & ~3 | (i & 1) << 1 | (i >> 1) & 1) if k % 2 else i

    pairs = [(place(i, k) * blocks + k, place(target(i), k) * blocks + k) for i in range(n) for k in range(blocks)]
    return lax.ppermute(value, ("ep", "corner"), pairs)


def tiles(x):
    c, e = x.shape
    return x.reshape(c, e // LANES, LANES).transpose(1, 0, 2).reshape(-1, LANES)


def on_device(required, arrival, hold_required, early_arrival, part_ids, bin_edges):
    C, rows = required.shape
    bins = bin_edges.shape[0]
    n = lax.axis_size("ep")
    me = turned(lax.axis_index("ep"), lax.axis_index("corner") % 2 == 1)
    endpoints = rows * n
    density = GROUPS * bins / endpoints
    half = C // 2
    side = me % 2
    place = me // 2
    rest = n // 2
    data = (tiles(required), tiles(arrival), tiles(early_arrival), tiles(hold_required))
    ids = part_ids.reshape(-1, LANES)
    lines = ids.shape[0]
    coarse, fine, near, keep, send = run_prep(bin_edges, side.reshape(1), ids, *data, C)
    got = moved(send, lambda i: i ^ 1)
    prior = run_hist(place.reshape(1), coarse, fine, keep, half)
    chunks = run_hist(place.reshape(1), coarse, fine, got, half, rest, prior)
    shares = [rotate(near, "corner", d) for d in range(1, lax.axis_size("corner"))]

    own = GROUPS // rest
    nblk = bins // LANES
    each = C * nblk
    hrows = own * each
    total = chunks[0]
    row = lax.broadcasted_iota(jnp.int32, total.shape, 0)
    lane = lax.broadcasted_iota(jnp.int32, total.shape, 1)
    least = (row >= hrows) & (row < hrows + 2 * half) & (lane >= GROUPS)
    order = sorted(range(1, rest), key=lambda d: (-(d & -2), d))
    for d in order:
        piece = moved(chunks[d], lambda i: i ^ 2 * d)
        total = jnp.where(least, jnp.minimum(total, piece), total + piece)
    mine = jnp.where(row < hrows, total * density, total)
    pieces = [mine] + [None] * (n - 1)
    for d in range(1, rest):
        pieces[2 * d] = moved(mine, lambda i: i ^ 2 * d)
    pieces[1] = moved(mine, lambda i: i ^ 1)
    for d in range(1, rest):
        pieces[2 * d + 1] = moved(pieces[2 * d], lambda i: i ^ 1)
    worst = functools.reduce(jnp.minimum, shares, near)
    worst = worst.reshape(lines, 2, LANES)
    worst = worst.transpose(1, 0, 2).reshape(2, rows)
    full, part_tns, part_share, tns, wns = run_final(me.reshape(1), pieces, C, own, 2 * each, endpoints)
    part_hist = full.reshape(GROUPS, C, nblk, 2, LANES).transpose(0, 1, 3, 2, 4).reshape(GROUPS, C, 2, bins)
    part_tns = part_tns.transpose(2, 0, 1)
    part_share = part_share.reshape(GROUPS)
    return (part_hist, part_tns, part_share, tns, wns, worst)


def solution(mesh):
    in_specs = (
        P("corner", "ep"),
        P("corner", "ep"),
        P("corner", "ep"),
        P("corner", "ep"),
        P("ep"),
        P(),
    )
    out_specs = (
        P(None, "corner", None, None),
        P(None, "corner", None),
        P(),
        P("corner", None),
        P("corner", None),
        P(None, "ep"),
    )
    return jax.shard_map(
        on_device, mesh=mesh, in_specs=in_specs, out_specs=out_specs, check_vma=False
    )
```

```python
import functools
import jax
import jax.numpy as jnp
from jax import lax
from jax.experimental import pallas as pl
from jax.experimental.pallas import tpu as pltpu
from jax.sharding import PartitionSpec as P

GROUPS = 64
LANES = 128
LEAST = 4096
F8 = jnp.float8_e4m3fn
BF = jnp.bfloat16
STEP = 0.001
VMEM = 12 << 20
EXTRA = 8


def lookup(table_ref, index):
    lane = index & (LANES - 1)
    row = index >> 7
    out = None
    for r in range(table_ref.shape[0]):
        line = jnp.broadcast_to(table_ref[r:r + 1, :], index.shape)
        got = jnp.take_along_axis(line, lane, axis=1, mode="promise_in_bounds")
        out = got if out is None else jnp.where(row == r, got, out)
    return out


def interval(slack, x0, coarse_ref, fine_ref):
    t = jnp.minimum(jnp.maximum(slack, x0), 0.0)
    whole = jnp.floor(t * 1000.0)
    whole = jnp.where(t >= (whole + 1.0) * jnp.float32(STEP), whole + 1.0, whole)
    whole = jnp.where(t < whole * jnp.float32(STEP), whole - 1.0, whole)
    q = jnp.minimum(whole.astype(jnp.int32) + LEAST, LEAST - 1)
    cell = lookup(coarse_ref, q >> 3)
    upto = jnp.left_shift(2, q & 7) - 1
    j = (cell & 0xFFFF) + lax.population_count((cell >> 16) & upto) - 1
    pair = lookup(fine_ref, j)
    k = (pair & 0xFFFF) - LEAST
    x = k.astype(jnp.float32) * jnp.float32(STEP)
    xn = (k + (pair >> 16)).astype(jnp.float32) * jnp.float32(STEP)
    r = 1.0 / (xn - x)
    w1 = jnp.maximum((xn - t) * r, 0.0)
    w2 = jnp.maximum((t - x) * r, 0.0)
    local = j & (LANES - 1)
    odd = (j & 1) == 1
    even_place = ((local + 1) & ~1).astype(jnp.float32)
    odd_place = (local | 1).astype(jnp.float32)
    return (
        even_place,
        odd_place,
        jnp.where(odd, w2, w1),
        jnp.where(odd, w1, w2),
        (j >> 7).astype(jnp.float32),
        jnp.minimum(slack, 0.0),
    )


def prep_kernel(C, side_ref, *refs):
    sources, refs = refs[:6], refs[6:]
    (coarse_ref, fine_ref, worst_ref, keep_ref, send_ref), held, sems = refs[:5], refs[5:11], refs[11]
    copies = [pltpu.make_async_copy(src, dst, sems.at[i]) for i, (src, dst) in enumerate(zip(sources, held))]
    for copy in copies:
        copy.start()
    lines_ref, ids_ref, a_ref, b_ref, c_ref, d_ref = held
    copies[0].wait()
    lane = lax.broadcasted_iota(jnp.int32, (8, LANES), 1)
    counts = [jnp.zeros((8, LANES), jnp.int32) for _ in range(coarse_ref.shape[0])]
    for r in range(lines_ref.shape[0]):
        nodes = jnp.broadcast_to(lines_ref[r:r + 1, :] + LEAST, (LANES, LANES)).T
        for g in range(LANES // 8):
            node = nodes[g * 8:g * 8 + 8]
            here, bit = node >> 3, jnp.left_shift(65536, node & 7)
            for i in range(len(counts)):
                cell = lane + i * LANES
                counts[i] = counts[i] + jnp.where(here < cell, 1, jnp.where(here == cell, bit, 0))
    for i, count in enumerate(counts):
        coarse_ref[i:i + 1, :] = jnp.sum(count, axis=0, keepdims=True)
    q = lines_ref[...] + LEAST
    _, lanes = q.shape
    left = pltpu.roll(q, lanes - 1, 1)
    below = jnp.concatenate([left[1:], jnp.full((1, lanes), LEAST, jnp.int32)], axis=0)
    last = lax.broadcasted_iota(jnp.int32, q.shape, 1) == lanes - 1
    following = jnp.where(last, below, left)
    fine_ref[...] = q + (following - q) * 65536

    for copy in copies[1:]:
        copy.wait()
    flag = side_ref[0] == 0
    half = C // 2
    lines = a_ref.shape[0] // C
    for m, (late, early) in enumerate(((a_ref, b_ref), (c_ref, d_ref))):
        for k in range(half):
            pieces = []
            for c in (k, k + half):
                at = pl.ds(c, lines, stride=C)
                pieces.append(late[at, :] - early[at, :])
            keep_ref[m, pl.ds(k, lines, stride=half), :] = jnp.where(flag, pieces[0], pieces[1])
            send_ref[m, pl.ds(k, lines, stride=half), :] = jnp.where(flag, pieces[1], pieces[0])
            for piece in pieces:
                first = k == 0 and piece is pieces[0]
                at = pl.ds(m, lines, stride=2)
                worst_ref[at, :] = piece if first else jnp.minimum(worst_ref[at, :], piece)
    ids = ids_ref[...].astype(jnp.float32)
    keep_ref[2, :lines, :] = ids
    send_ref[2, :lines, :] = ids


def run_prep(edges, side, ids, a, b, c, d, C):
    bins = edges.shape[0]
    lines = ids.shape[0]
    sources = (edges.reshape(-1, LANES), ids, a, b, c, d)
    sources = [pltpu.with_memory_space_constraint(x, pltpu.HBM) for x in sources]
    held = [pltpu.VMEM(x.shape, x.dtype) for x in sources]
    return pl.pallas_call(
        functools.partial(prep_kernel, C),
        in_specs=[pl.BlockSpec(memory_space=pltpu.SMEM)] + [pl.BlockSpec(memory_space=pltpu.HBM)] * 6,
        out_shape=[
            jax.ShapeDtypeStruct((LEAST // 8 // LANES, LANES), jnp.int32),
            jax.ShapeDtypeStruct((bins // LANES, LANES), jnp.int32),
            jax.ShapeDtypeStruct((2 * lines, LANES), jnp.float32),
            jax.ShapeDtypeStruct((3, lines * C // 2, LANES), jnp.float32),
            jax.ShapeDtypeStruct((3, lines * C // 2, LANES), jnp.float32),
        ],
        scratch_shapes=held + [pltpu.SemaphoreType.DMA((6,))],
        compiler_params=pltpu.CompilerParams(vmem_limit_bytes=VMEM),
        name="prep",
    )(side, *sources)


def hist_kernel(C, KT, n, place_ref, coarse_ref, fine_ref, slack_ref, *refs):
    if n:
        prior_ref, prior_low_ref = refs[:2]
        outs, (low_ref, buf0, buf1, zed0, zed1, all_ref) = refs[2:2 + n], refs[2 + n:]
    else:
        out_ref, low_ref, buf0, buf1, zed0, zed1 = refs
    series = 2 * C
    nblk = fine_ref.shape[0]
    lines = KT * C
    chunks = slack_ref.shape[1] // lines
    x0 = ((fine_ref[:1, :1] & 0xFFFF) - LEAST).astype(jnp.float32) * jnp.float32(STEP)

    def body(*refs):
        for a in refs:
            pltpu.matmul_pop(a)
        accs, zaccs = refs[:series], refs[series:]
        iota16 = lax.broadcasted_iota(jnp.int32, (16, LANES), 0)
        iotas = [(iota16 + 16 * v).astype(jnp.float32).astype(BF) for v in range(LANES // 16)]
        iota32 = lax.broadcasted_iota(jnp.int32, (32, LANES), 0)
        iotas32 = [(iota32 + 32 * v).astype(jnp.float32).astype(BF) for v in range(GROUPS // 32)]
        even = (iota16 & 1) == 0
        iota8 = lax.broadcasted_iota(jnp.int32, (8, LANES), 0)
        one = jnp.ones((32, LANES), jnp.float32).astype(F8)
        zero16 = jnp.zeros((16, LANES), BF)
        none = jnp.zeros((32, LANES), F8)
        blank = jnp.where(iota8 == 3, 1.0, 0.0)

        def wide(x, rows):
            return jnp.broadcast_to(x, (rows, LANES))

        def look(buf, zed, chunk, g):
            start = pl.multiple_of(chunk * lines + g * 8, 8)
            at = pl.ds(start, 8)
            for m in range(2):
                slack = slack_ref[m, at, :]
                low_ref[m] = jnp.minimum(low_ref[m], slack)
                found = interval(slack, x0, coarse_ref, fine_ref)
                for i, v in enumerate(found[:5]):
                    buf[i, m, g * 8:g * 8 + 8, :] = v
                high = found[5].astype(BF).astype(jnp.float32)
                cross = jnp.where(found[0] == float(LANES), found[2], 0.0)
                parts = {0: high, 1: found[5] - high}
                for h in range(nblk - 1):
                    parts[4 + h] = jnp.where(found[4] == float(h), cross, 0.0)
                for i, v in parts.items():
                    zed[m, pl.ds(g * 64 + i, 8, stride=8), :] = v

        def pair(buf, zed, chunk, k2):
            member = []
            for kk in range(2):
                ids = wide(slack_ref[2, pl.ds(chunk * KT + 2 * k2 + kk, 1), :], 32).astype(BF)
                member.append([jnp.where(i == ids, one, none) for i in iotas32])
            for s in range(series):
                c, m = divmod(s, 2)
                left, right = [], []
                for kk in range(2):
                    r = (2 * k2 + kk) * C + c
                    row = [buf[i, m, r:r + 1, :] for i in range(5)]
                    block = wide(row[4], 32).astype(BF)
                    left.append(jnp.concatenate([
                        jnp.where(block == jnp.bfloat16(h), part, none) for h in range(nblk) for part in member[kk]
                    ], axis=0))
                    place = jnp.where(even, wide(row[0], 16), wide(row[1], 16)).astype(BF)
                    weight = jnp.where(even, wide(row[2], 16), wide(row[3], 16)).astype(BF)
                    hats = [jnp.where(i == place, weight, zero16) for i in iotas]
                    right.append(jnp.concatenate(hats, axis=0))
                pltpu.matmul_push_rhs(
                    jnp.concatenate(left, axis=1), staging_register=0, mxu_index=s % 2, transpose=True
                )
                pltpu.matmul_acc_lhs(accs[s], jnp.concatenate(right, axis=1), load_staged_rhs=0)
                if m == k2 % 2:
                    extra = []
                    for kk in range(2):
                        r = (2 * k2 + kk) * C + c
                        both_kinds = [zed[i, r * 8:r * 8 + 8, :] for i in (m, 1 - m)]
                        extra.append(jnp.concatenate(both_kinds, axis=0).astype(BF))
                    pltpu.matmul_acc_lhs(zaccs[s], jnp.concatenate(extra, axis=1))

        def both(chunk, buf, zed, ahead, other, other_zed):
            pairs, groups = KT // 2, lines // 8
            done = 0
            for k2 in range(pairs):
                pair(buf, zed, chunk, k2)
                while done < groups and done * pairs <= k2 * groups:
                    look(other, other_zed, ahead, done)
                    done += 1

        low_ref[...] = prior_low_ref[...] if n else jnp.full(low_ref.shape, jnp.inf)
        for zed in (zed0, zed1):
            for m in range(2):
                for r in range(lines):
                    zed[m, r * 8:r * 8 + 8, :] = blank
        for g in range(lines // 8):
            look(buf0, zed0, 0, g)

        def two(i, carry):
            both(2 * i, buf0, zed0, 2 * i + 1, buf1, zed1)
            both(2 * i + 1, buf1, zed1, jnp.minimum(2 * i + 2, chunks - 1), buf0, zed0)
            return carry

        lax.fori_loop(0, chunks // 2, two, 0)

        sums = [pltpu.matmul_pop(a) for a in accs]
        zeds = [pltpu.matmul_pop(a) for a in zaccs]
        if not n:
            for s in range(series):
                out_ref[s, :LANES] = sums[s]
                out_ref[s, LANES:] = zeds[s]
            return
        zeds = [prior_ref[s, LANES:] + zeds[s] for s in range(series)]
        own = GROUPS // n
        lane = lax.broadcasted_iota(jnp.int32, (8, LANES), 1)
        sub = lax.broadcasted_iota(jnp.int32, (8, LANES), 0)
        wide_lane = lax.broadcasted_iota(jnp.int32, (8, nblk * GROUPS), 1)
        wide_sub = lax.broadcasted_iota(jnp.int32, (8, nblk * GROUPS), 0)
        chunk_rows = outs[0].shape[0]
        hist_rows = own * series * nblk
        tile = jnp.zeros((8, LANES), jnp.float32)
        for s in range(series):
            c, m = divmod(s, 2)
            total = prior_ref[s, :LANES] + sums[s]
            stats = zeds[s][:8] + zeds[s ^ 1][8:]
            folded = stats[:, :LANES]
            for v in range(1, nblk * GROUPS // LANES):
                folded = folded + stats[:, v * LANES:(v + 1) * LANES]
            folded = folded + pltpu.roll(folded, GROUPS, 1)
            passed = jnp.where(lane < GROUPS, 0.0, folded[4:5])[:1]
            passed = [passed] + [
                jnp.where(lane < GROUPS, folded[2 * v + 3:2 * v + 4], folded[2 * v + 4:2 * v + 5])[:1]
                for v in range(1, nblk * GROUPS // LANES)
            ]
            across = jnp.broadcast_to(jnp.concatenate(passed, axis=1), wide_lane.shape)
            top = total[:8] + jnp.where((wide_sub == 0) & (wide_lane >= GROUPS), across, 0.0)
            full = jnp.concatenate([top, total[8:LANES]], axis=0).T
            low = jnp.min(jnp.where(sub % C == c, low_ref[m], jnp.inf), keepdims=True)
            row = jnp.where(lane < GROUPS, folded[0:1] + folded[1:2], low)
            tile = jnp.where(sub == s, row, tile)
            if s == 0:
                tile = jnp.where(sub == series, folded[3:4], tile)
            for h in range(nblk):
                for i in range(n):
                    at = i * chunk_rows + (c * nblk + h) * 2 + m
                    first = h * GROUPS + i * own
                    all_ref[pl.ds(at, own, stride=series * nblk), :] = full[first:first + own]
        for i in range(n):
            at = i * chunk_rows + hist_rows
            all_ref[at:at + EXTRA, :] = tile
        for d in range(n):
            at = pl.multiple_of((place_ref[0] ^ d) * chunk_rows, 8)
            outs[d][...] = all_ref[pl.ds(at, chunk_rows), :]

    shapes = [(LANES, nblk * GROUPS)] * series + [(16, nblk * GROUPS)] * series
    pl.run_scoped(body, *[pltpu.ACC(i % 2)(shape, jnp.float32) for i, shape in enumerate(shapes)])


def run_hist(place, coarse, fine, slack, C, n=0, prior=(), KT=32):
    nblk = fine.shape[0]
    series = 2 * C
    smem = pl.BlockSpec(memory_space=pltpu.SMEM)
    vm = pl.BlockSpec(memory_space=pltpu.VMEM)
    scratch = [pltpu.VMEM((5, 2, KT * C, LANES), jnp.float32) for _ in range(2)]
    scratch += [pltpu.VMEM((2, KT * C * 8, LANES), jnp.float32) for _ in range(2)]
    low = jax.ShapeDtypeStruct((2, 8, LANES), jnp.float32)
    if n:
        own = GROUPS // n
        rows = own * series * nblk + EXTRA
        outs = [jax.ShapeDtypeStruct((rows, LANES), jnp.float32) for _ in range(n)]
        scratch += [pltpu.VMEM((2, 8, LANES), jnp.float32)] * 0 + [pltpu.VMEM((n * rows, LANES), jnp.float32)]
    else:
        outs = [jax.ShapeDtypeStruct((series, LANES + 16, nblk * GROUPS), jnp.float32)]
    return pl.pallas_call(
        functools.partial(hist_kernel, C, KT, n),
        in_specs=[smem] + [vm] * (3 + len(prior)),
        out_shape=outs + [low],
        scratch_shapes=scratch,
        cost_estimate=pl.CostEstimate(
            flops=4 * (LANES + 16) * 256 * slack.size // 3, bytes_accessed=8 * slack.size, transcendentals=slack.size
        ),
        compiler_params=pltpu.CompilerParams(vmem_limit_bytes=VMEM),
        name="hist",
    )(place, coarse, fine, slack, *prior)


def final_kernel(C, own, share, scale, me_ref, *refs):
    n = len(refs) - 5
    pieces = refs[:n]
    hist_ref, part_ref, share_ref, tns_ref, wns_ref = refs[n:]
    half = C // 2
    each = hist_ref.shape[0] // GROUPS // 2
    for d in range(n):
        source = me_ref[0] ^ d
        place, side = source >> 1, source & 1
        for p in range(own):
            at = pl.multiple_of((place * own + p) * 2 * each + side * each, 8)
            hist_ref[pl.ds(at, each), :] = pieces[d][p * each:(p + 1) * each, :]
    tns = jnp.zeros((C, 2), jnp.float32)
    wns = jnp.zeros((C, 2), jnp.float32)
    row = lax.broadcasted_iota(jnp.int32, (C, 2), 0)
    col = lax.broadcasted_iota(jnp.int32, (C, 2), 1)
    mine, other = pieces[0][own * each:, :], pieces[1][own * each:, :]
    even = me_ref[0] % 2 == 0
    for side in range(2):
        tile = jnp.where(even, mine, other) if side == 0 else jnp.where(even, other, mine)
        for s in range(2 * half):
            c, m = divmod(s, 2)
            c += side * half
            sums = tile[s:s + 1, :GROUPS]
            part_ref[c, m:m + 1, :] = sums * share
            here = (row == c) & (col == m)
            tns = jnp.where(here, jnp.sum(sums, keepdims=True) * scale, tns)
            wns = jnp.where(here, tile[s:s + 1, GROUPS:GROUPS + 1], wns)
    share_ref[...] = mine[2 * half:2 * half + 1, :GROUPS] * share
    tns_ref[...] = tns
    wns_ref[...] = wns


def run_final(me, pieces, C, own, rows, endpoints):
    vm = pl.BlockSpec(memory_space=pltpu.VMEM)
    return pl.pallas_call(
        functools.partial(final_kernel, C, own, GROUPS / endpoints, 1.0 / endpoints),
        in_specs=[pl.BlockSpec(memory_space=pltpu.SMEM)] + [vm] * len(pieces),
        out_shape=[
            jax.ShapeDtypeStruct((GROUPS * rows, LANES), jnp.float32),
            jax.ShapeDtypeStruct((C, 2, GROUPS), jnp.float32),
            jax.ShapeDtypeStruct((1, GROUPS), jnp.float32),
            jax.ShapeDtypeStruct((C, 2), jnp.float32),
            jax.ShapeDtypeStruct((C, 2), jnp.float32),
        ],
        compiler_params=pltpu.CompilerParams(vmem_limit_bytes=VMEM),
        name="final",
    )(me, *pieces)


def rotate(value, axis, distance):
    size = lax.axis_size(axis)
    return lax.ppermute(value, axis, [(i, (i + distance) % size) for i in range(size)])


def turned(index, odd):
    return jnp.where(odd, (index & ~3) | ((index & 1) << 1) | ((index >> 1) & 1), index)


def moved(value, target):
    n, blocks = lax.axis_size("ep"), lax.axis_size("corner")

    def place(i, k):
        return (i & ~3 | (i & 1) << 1 | (i >> 1) & 1) if k % 2 else i

    pairs = [(place(i, k) * blocks + k, place(target(i), k) * blocks + k) for i in range(n) for k in range(blocks)]
    return lax.ppermute(value, ("ep", "corner"), pairs)


def tiles(x):
    c, e = x.shape
    return x.reshape(c, e // LANES, LANES).transpose(1, 0, 2).reshape(-1, LANES)


def on_device(required, arrival, hold_required, early_arrival, part_ids, bin_edges):
    C, rows = required.shape
    bins = bin_edges.shape[0]
    n = lax.axis_size("ep")
    me = turned(lax.axis_index("ep"), lax.axis_index("corner") % 2 == 1)
    endpoints = rows * n
    density = GROUPS * bins / endpoints
    half = C // 2
    side = me % 2
    place = me // 2
    rest = n // 2
    data = (tiles(required), tiles(arrival), tiles(early_arrival), tiles(hold_required))
    ids = part_ids.reshape(-1, LANES)
    lines = ids.shape[0]
    coarse, fine, near, keep, send = run_prep(bin_edges, side.reshape(1), ids, *data, C)
    got = moved(send, lambda i: i ^ 1)
    prior = run_hist(place.reshape(1), coarse, fine, keep, half)
    chunks = run_hist(place.reshape(1), coarse, fine, got, half, rest, prior)
    shares = [rotate(near, "corner", d) for d in range(1, lax.axis_size("corner"))]

    own = GROUPS // rest
    nblk = bins // LANES
    each = C * nblk
    hrows = own * each
    total = chunks[0]
    row = lax.broadcasted_iota(jnp.int32, total.shape, 0)
    lane = lax.broadcasted_iota(jnp.int32, total.shape, 1)
    least = (row >= hrows) & (row < hrows + 2 * half) & (lane >= GROUPS)
    order = sorted(range(1, rest), key=lambda d: (d != rest // 2, d))
    for d in order:
        piece = moved(chunks[d], lambda i: i ^ 2 * d)
        total = jnp.where(least, jnp.minimum(total, piece), total + piece)
    mine = jnp.where(row < hrows, total * density, total)
    pieces = [mine] + [None] * (n - 1)
    for d in range(1, rest):
        pieces[2 * d] = moved(mine, lambda i: i ^ 2 * d)
    pieces[1] = moved(mine, lambda i: i ^ 1)
    for d in range(1, rest):
        pieces[2 * d + 1] = moved(pieces[2 * d], lambda i: i ^ 1)
    worst = functools.reduce(jnp.minimum, shares, near)
    worst = worst.reshape(lines, 2, LANES)
    worst = worst.transpose(1, 0, 2).reshape(2, rows)
    full, part_tns, part_share, tns, wns = run_final(me.reshape(1), pieces, C, own, 2 * each, endpoints)
    part_hist = full.reshape(GROUPS, C, nblk, 2, LANES).transpose(0, 1, 3, 2, 4).reshape(GROUPS, C, 2, bins)
    part_tns = part_tns.transpose(2, 0, 1)
    part_share = part_share.reshape(GROUPS)
    return (part_hist, part_tns, part_share, tns, wns, worst)


def solution(mesh):
    in_specs = (
        P("corner", "ep"),
        P("corner", "ep"),
        P("corner", "ep"),
        P("corner", "ep"),
        P("ep"),
        P(),
    )
    out_specs = (
        P(None, "corner", None, None),
        P(None, "corner", None),
        P(),
        P("corner", None),
        P("corner", None),
        P(None, "ep"),
    )
    return jax.shard_map(
        on_device, mesh=mesh, in_specs=in_specs, out_specs=out_specs, check_vma=False
    )
```

```python
import functools
import jax
import jax.numpy as jnp
from jax import lax
from jax.experimental import pallas as pl
from jax.experimental.pallas import tpu as pltpu
from jax.sharding import PartitionSpec as P

GROUPS = 64
LANES = 128
LEAST = 4096
F8 = jnp.float8_e4m3fn
BF = jnp.bfloat16
STEP = 0.001
VMEM = 12 << 20
EXTRA = 8


def lookup(table_ref, index):
    lane = index & (LANES - 1)
    row = index >> 7
    out = None
    for r in range(table_ref.shape[0]):
        line = jnp.broadcast_to(table_ref[r:r + 1, :], index.shape)
        got = jnp.take_along_axis(line, lane, axis=1, mode="promise_in_bounds")
        out = got if out is None else jnp.where(row == r, got, out)
    return out


def interval(slack, x0, coarse_ref, fine_ref):
    t = jnp.minimum(jnp.maximum(slack, x0), 0.0)
    whole = jnp.floor(t * 1000.0)
    whole = jnp.where(t >= (whole + 1.0) * jnp.float32(STEP), whole + 1.0, whole)
    whole = jnp.where(t < whole * jnp.float32(STEP), whole - 1.0, whole)
    q = jnp.minimum(whole.astype(jnp.int32) + LEAST, LEAST - 1)
    cell = lookup(coarse_ref, q >> 3)
    upto = jnp.left_shift(2, q & 7) - 1
    j = (cell & 0xFFFF) + lax.population_count((cell >> 16) & upto) - 1
    pair = lookup(fine_ref, j)
    k = (pair & 0xFFFF) - LEAST
    x = k.astype(jnp.float32) * jnp.float32(STEP)
    xn = (k + (pair >> 16)).astype(jnp.float32) * jnp.float32(STEP)
    r = 1.0 / (xn - x)
    w1 = jnp.maximum((xn - t) * r, 0.0)
    w2 = jnp.maximum((t - x) * r, 0.0)
    local = j & (LANES - 1)
    odd = (j & 1) == 1
    even_place = ((local + 1) & ~1).astype(jnp.float32)
    odd_place = (local | 1).astype(jnp.float32)
    return (
        even_place,
        odd_place,
        jnp.where(odd, w2, w1),
        jnp.where(odd, w1, w2),
        (j >> 7).astype(jnp.float32),
        jnp.minimum(slack, 0.0),
    )


def prep_kernel(C, side_ref, *refs):
    sources, refs = refs[:6], refs[6:]
    (coarse_ref, fine_ref, worst_ref, keep_ref, send_ref), held, sems = refs[:5], refs[5:11], refs[11]
    copies = [pltpu.make_async_copy(src, dst, sems.at[i]) for i, (src, dst) in enumerate(zip(sources, held))]
    for copy in copies:
        copy.start()
    lines_ref, ids_ref, a_ref, b_ref, c_ref, d_ref = held
    copies[0].wait()
    lane = lax.broadcasted_iota(jnp.int32, (8, LANES), 1)
    counts = [jnp.zeros((8, LANES), jnp.int32) for _ in range(coarse_ref.shape[0])]
    for r in range(lines_ref.shape[0]):
        nodes = jnp.broadcast_to(lines_ref[r:r + 1, :] + LEAST, (LANES, LANES)).T
        for g in range(LANES // 8):
            node = nodes[g * 8:g * 8 + 8]
            here, bit = node >> 3, jnp.left_shift(65536, node & 7)
            for i in range(len(counts)):
                cell = lane + i * LANES
                counts[i] = counts[i] + jnp.where(here < cell, 1, jnp.where(here == cell, bit, 0))
    for i, count in enumerate(counts):
        coarse_ref[i:i + 1, :] = jnp.sum(count, axis=0, keepdims=True)
    q = lines_ref[...] + LEAST
    _, lanes = q.shape
    left = pltpu.roll(q, lanes - 1, 1)
    below = jnp.concatenate([left[1:], jnp.full((1, lanes), LEAST, jnp.int32)], axis=0)
    last = lax.broadcasted_iota(jnp.int32, q.shape, 1) == lanes - 1
    following = jnp.where(last, below, left)
    fine_ref[...] = q + (following - q) * 65536

    for copy in copies[1:]:
        copy.wait()
    flag = side_ref[0] == 0
    half = C // 2
    lines = a_ref.shape[0] // C
    for m, (late, early) in enumerate(((a_ref, b_ref), (c_ref, d_ref))):
        for k in range(half):
            pieces = []
            for c in (k, k + half):
                at = pl.ds(c, lines, stride=C)
                pieces.append(late[at, :] - early[at, :])
            keep_ref[m, pl.ds(k, lines, stride=half), :] = jnp.where(flag, pieces[0], pieces[1])
            send_ref[m, pl.ds(k, lines, stride=half), :] = jnp.where(flag, pieces[1], pieces[0])
            for piece in pieces:
                first = k == 0 and piece is pieces[0]
                at = pl.ds(m, lines, stride=2)
                worst_ref[at, :] = piece if first else jnp.minimum(worst_ref[at, :], piece)
    ids = ids_ref[...].astype(jnp.float32)
    keep_ref[2, :lines, :] = ids
    send_ref[2, :lines, :] = ids


def run_prep(edges, side, ids, a, b, c, d, C):
    bins = edges.shape[0]
    lines = ids.shape[0]
    sources = (edges.reshape(-1, LANES), ids, a, b, c, d)
    sources = [pltpu.with_memory_space_constraint(x, pltpu.HBM) for x in sources]
    held = [pltpu.VMEM(x.shape, x.dtype) for x in sources]
    return pl.pallas_call(
        functools.partial(prep_kernel, C),
        in_specs=[pl.BlockSpec(memory_space=pltpu.SMEM)] + [pl.BlockSpec(memory_space=pltpu.HBM)] * 6,
        out_shape=[
            jax.ShapeDtypeStruct((LEAST // 8 // LANES, LANES), jnp.int32),
            jax.ShapeDtypeStruct((bins // LANES, LANES), jnp.int32),
            jax.ShapeDtypeStruct((2 * lines, LANES), jnp.float32),
            jax.ShapeDtypeStruct((3, lines * C // 2, LANES), jnp.float32),
            jax.ShapeDtypeStruct((3, lines * C // 2, LANES), jnp.float32),
        ],
        scratch_shapes=held + [pltpu.SemaphoreType.DMA((6,))],
        compiler_params=pltpu.CompilerParams(vmem_limit_bytes=VMEM),
        name="prep",
    )(side, *sources)


def hist_kernel(C, KT, n, place_ref, coarse_ref, fine_ref, slack_ref, *refs):
    if n:
        prior_ref, prior_low_ref = refs[:2]
        outs, (low_ref, buf0, buf1, zed0, zed1, all_ref) = refs[2:2 + n], refs[2 + n:]
    else:
        out_ref, low_ref, buf0, buf1, zed0, zed1 = refs
    series = 2 * C
    nblk = fine_ref.shape[0]
    lines = KT * C
    chunks = slack_ref.shape[1] // lines
    x0 = ((fine_ref[:1, :1] & 0xFFFF) - LEAST).astype(jnp.float32) * jnp.float32(STEP)

    def body(*refs):
        for a in refs:
            pltpu.matmul_pop(a)
        accs, zaccs = refs[:series], refs[series:]
        iota16 = lax.broadcasted_iota(jnp.int32, (16, LANES), 0)
        iotas = [(iota16 + 16 * v).astype(jnp.float32).astype(BF) for v in range(LANES // 16)]
        iota32 = lax.broadcasted_iota(jnp.int32, (32, LANES), 0)
        iotas32 = [(iota32 + 32 * v).astype(jnp.float32).astype(BF) for v in range(GROUPS // 32)]
        even = (iota16 & 1) == 0
        iota8 = lax.broadcasted_iota(jnp.int32, (8, LANES), 0)
        one = jnp.ones((32, LANES), jnp.float32).astype(F8)
        zero16 = jnp.zeros((16, LANES), BF)
        none = jnp.zeros((32, LANES), F8)
        blank = jnp.where(iota8 == 3, 1.0, 0.0)

        def wide(x, rows):
            return jnp.broadcast_to(x, (rows, LANES))

        def look(buf, zed, chunk, g):
            start = pl.multiple_of(chunk * lines + g * 8, 8)
            at = pl.ds(start, 8)
            for m in range(2):
                slack = slack_ref[m, at, :]
                low_ref[m] = jnp.minimum(low_ref[m], slack)
                found = interval(slack, x0, coarse_ref, fine_ref)
                for i, v in enumerate(found[:5]):
                    buf[i, m, g * 8:g * 8 + 8, :] = v
                high = found[5].astype(BF).astype(jnp.float32)
                cross = jnp.where(found[0] == float(LANES), found[2], 0.0)
                parts = {0: high, 1: found[5] - high}
                for h in range(nblk - 1):
                    parts[4 + h] = jnp.where(found[4] == float(h), cross, 0.0)
                for i, v in parts.items():
                    zed[m, pl.ds(g * 64 + i, 8, stride=8), :] = v

        def pair(buf, zed, chunk, k2):
            member = []
            for kk in range(2):
                ids = wide(slack_ref[2, pl.ds(chunk * KT + 2 * k2 + kk, 1), :], 32).astype(BF)
                member.append([jnp.where(i == ids, one, none) for i in iotas32])
            for s in range(series):
                c, m = divmod(s, 2)
                left, right = [], []
                for kk in range(2):
                    r = (2 * k2 + kk) * C + c
                    row = [buf[i, m, r:r + 1, :] for i in range(5)]
                    block = wide(row[4], 32).astype(BF)
                    left.append(jnp.concatenate([
                        jnp.where(block == jnp.bfloat16(h), part, none) for h in range(nblk) for part in member[kk]
                    ], axis=0))
                    place = jnp.where(even, wide(row[0], 16), wide(row[1], 16)).astype(BF)
                    weight = jnp.where(even, wide(row[2], 16), wide(row[3], 16)).astype(BF)
                    hats = [jnp.where(i == place, weight, zero16) for i in iotas]
                    right.append(jnp.concatenate(hats, axis=0))
                pltpu.matmul_push_rhs(
                    jnp.concatenate(left, axis=1), staging_register=0, mxu_index=s % 2, transpose=True
                )
                pltpu.matmul_acc_lhs(accs[s], jnp.concatenate(right, axis=1), load_staged_rhs=0)
                if m == k2 % 2:
                    extra = []
                    for kk in range(2):
                        r = (2 * k2 + kk) * C + c
                        both_kinds = [zed[i, r * 8:r * 8 + 8, :] for i in (m, 1 - m)]
                        extra.append(jnp.concatenate(both_kinds, axis=0).astype(BF))
                    pltpu.matmul_acc_lhs(zaccs[s], jnp.concatenate(extra, axis=1))

        def both(chunk, buf, zed, ahead, other, other_zed):
            pairs, groups = KT // 2, lines // 8
            done = 0
            for k2 in range(pairs):
                pair(buf, zed, chunk, k2)
                while done < groups and done * pairs <= k2 * groups:
                    look(other, other_zed, ahead, done)
                    done += 1

        low_ref[...] = prior_low_ref[...] if n else jnp.full(low_ref.shape, jnp.inf)
        for zed in (zed0, zed1):
            for m in range(2):
                for r in range(lines):
                    zed[m, r * 8:r * 8 + 8, :] = blank
        for g in range(lines // 8):
            look(buf0, zed0, 0, g)

        def two(i, carry):
            both(2 * i, buf0, zed0, 2 * i + 1, buf1, zed1)
            both(2 * i + 1, buf1, zed1, jnp.minimum(2 * i + 2, chunks - 1), buf0, zed0)
            return carry

        lax.fori_loop(0, chunks // 2, two, 0)

        sums = [pltpu.matmul_pop(a) for a in accs]
        zeds = [pltpu.matmul_pop(a) for a in zaccs]
        if not n:
            for s in range(series):
                out_ref[s, :LANES] = sums[s]
                out_ref[s, LANES:] = zeds[s]
            return
        zeds = [prior_ref[s, LANES:] + zeds[s] for s in range(series)]
        own = GROUPS // n
        lane = lax.broadcasted_iota(jnp.int32, (8, LANES), 1)
        sub = lax.broadcasted_iota(jnp.int32, (8, LANES), 0)
        wide_lane = lax.broadcasted_iota(jnp.int32, (8, nblk * GROUPS), 1)
        wide_sub = lax.broadcasted_iota(jnp.int32, (8, nblk * GROUPS), 0)
        chunk_rows = outs[0].shape[0]
        hist_rows = own * series * nblk
        tile = jnp.zeros((8, LANES), jnp.float32)
        for s in range(series):
            c, m = divmod(s, 2)
            total = prior_ref[s, :LANES] + sums[s]
            stats = zeds[s][:8] + zeds[s ^ 1][8:]
            folded = stats[:, :LANES]
            for v in range(1, nblk * GROUPS // LANES):
                folded = folded + stats[:, v * LANES:(v + 1) * LANES]
            folded = folded + pltpu.roll(folded, GROUPS, 1)
            passed = jnp.where(lane < GROUPS, 0.0, folded[4:5])[:1]
            passed = [passed] + [
                jnp.where(lane < GROUPS, folded[2 * v + 3:2 * v + 4], folded[2 * v + 4:2 * v + 5])[:1]
                for v in range(1, nblk * GROUPS // LANES)
            ]
            across = jnp.broadcast_to(jnp.concatenate(passed, axis=1), wide_lane.shape)
            top = total[:8] + jnp.where((wide_sub == 0) & (wide_lane >= GROUPS), across, 0.0)
            full = jnp.concatenate([top, total[8:LANES]], axis=0).T
            low = jnp.min(jnp.where(sub % C == c, low_ref[m], jnp.inf), keepdims=True)
            row = jnp.where(lane < GROUPS, folded[0:1] + folded[1:2], low)
            tile = jnp.where(sub == s, row, tile)
            if s == 0:
                tile = jnp.where(sub == series, folded[3:4], tile)
            for h in range(nblk):
                for i in range(n):
                    at = i * chunk_rows + (c * nblk + h) * 2 + m
                    first = h * GROUPS + i * own
                    all_ref[pl.ds(at, own, stride=series * nblk), :] = full[first:first + own]
        for i in range(n):
            at = i * chunk_rows + hist_rows
            all_ref[at:at + EXTRA, :] = tile
        for d in range(n):
            at = pl.multiple_of((place_ref[0] ^ d) * chunk_rows, 8)
            outs[d][...] = all_ref[pl.ds(at, chunk_rows), :]

    shapes = [(LANES, nblk * GROUPS)] * series + [(16, nblk * GROUPS)] * series
    pl.run_scoped(body, *[pltpu.ACC(i % 2)(shape, jnp.float32) for i, shape in enumerate(shapes)])


def run_hist(place, coarse, fine, slack, C, n=0, prior=(), KT=32):
    nblk = fine.shape[0]
    series = 2 * C
    smem = pl.BlockSpec(memory_space=pltpu.SMEM)
    vm = pl.BlockSpec(memory_space=pltpu.VMEM)
    scratch = [pltpu.VMEM((5, 2, KT * C, LANES), jnp.float32) for _ in range(2)]
    scratch += [pltpu.VMEM((2, KT * C * 8, LANES), jnp.float32) for _ in range(2)]
    low = jax.ShapeDtypeStruct((2, 8, LANES), jnp.float32)
    if n:
        own = GROUPS // n
        rows = own * series * nblk + EXTRA
        outs = [jax.ShapeDtypeStruct((rows, LANES), jnp.float32) for _ in range(n)]
        scratch += [pltpu.VMEM((2, 8, LANES), jnp.float32)] * 0 + [pltpu.VMEM((n * rows, LANES), jnp.float32)]
    else:
        outs = [jax.ShapeDtypeStruct((series, LANES + 16, nblk * GROUPS), jnp.float32)]
    return pl.pallas_call(
        functools.partial(hist_kernel, C, KT, n),
        in_specs=[smem] + [vm] * (3 + len(prior)),
        out_shape=outs + [low],
        scratch_shapes=scratch,
        cost_estimate=pl.CostEstimate(
            flops=4 * (LANES + 16) * 256 * slack.size // 3, bytes_accessed=8 * slack.size, transcendentals=slack.size
        ),
        compiler_params=pltpu.CompilerParams(vmem_limit_bytes=VMEM),
        name="hist",
    )(place, coarse, fine, slack, *prior)


def final_kernel(own, me_ref, *refs):
    pieces, hist_ref = refs[:-1], refs[-1]
    n = len(pieces)
    each = hist_ref.shape[0] // GROUPS // 2
    for d in range(n):
        source = me_ref[0] ^ d
        place, side = source >> 1, source & 1
        for p in range(own):
            at = pl.multiple_of((place * own + p) * 2 * each + side * each, 8)
            hist_ref[pl.ds(at, each), :] = pieces[d][p * each:(p + 1) * each, :]


def small_kernel(C, share, scale, me_ref, mine_ref, other_ref, part_ref, share_ref, tns_ref, wns_ref):
    half = C // 2
    top = mine_ref.shape[0] - EXTRA
    tns = jnp.zeros((C, 2), jnp.float32)
    wns = jnp.zeros((C, 2), jnp.float32)
    row = lax.broadcasted_iota(jnp.int32, (C, 2), 0)
    col = lax.broadcasted_iota(jnp.int32, (C, 2), 1)
    mine, other = mine_ref[top:top + EXTRA, :], other_ref[top:top + EXTRA, :]
    even = me_ref[0] % 2 == 0
    for side in range(2):
        tile = jnp.where(even, mine, other) if side == 0 else jnp.where(even, other, mine)
        for s in range(2 * half):
            c, m = divmod(s, 2)
            c += side * half
            sums = tile[s:s + 1, :GROUPS]
            part_ref[c, m:m + 1, :] = sums * share
            here = (row == c) & (col == m)
            tns = jnp.where(here, jnp.sum(sums, keepdims=True) * scale, tns)
            wns = jnp.where(here, tile[s:s + 1, GROUPS:GROUPS + 1], wns)
    share_ref[...] = mine[2 * half:2 * half + 1, :GROUPS] * share
    tns_ref[...] = tns
    wns_ref[...] = wns


def run_final(me, pieces, own, rows):
    vm = pl.BlockSpec(memory_space=pltpu.VMEM)
    return pl.pallas_call(
        functools.partial(final_kernel, own),
        in_specs=[pl.BlockSpec(memory_space=pltpu.SMEM)] + [vm] * len(pieces),
        out_shape=jax.ShapeDtypeStruct((GROUPS * rows, LANES), jnp.float32),
        compiler_params=pltpu.CompilerParams(vmem_limit_bytes=VMEM),
        name="final",
    )(me, *pieces)


def run_small(me, mine, other, C, endpoints):
    vm = pl.BlockSpec(memory_space=pltpu.VMEM)
    return pl.pallas_call(
        functools.partial(small_kernel, C, GROUPS / endpoints, 1.0 / endpoints),
        in_specs=[pl.BlockSpec(memory_space=pltpu.SMEM), vm, vm],
        out_shape=[
            jax.ShapeDtypeStruct((C, 2, GROUPS), jnp.float32),
            jax.ShapeDtypeStruct((1, GROUPS), jnp.float32),
            jax.ShapeDtypeStruct((C, 2), jnp.float32),
            jax.ShapeDtypeStruct((C, 2), jnp.float32),
        ],
        compiler_params=pltpu.CompilerParams(vmem_limit_bytes=VMEM),
        name="small",
    )(me, mine, other)


def rotate(value, axis, distance):
    size = lax.axis_size(axis)
    return lax.ppermute(value, axis, [(i, (i + distance) % size) for i in range(size)])


def turned(index, odd):
    return jnp.where(odd, (index & ~3) | ((index & 1) << 1) | ((index >> 1) & 1), index)


def moved(value, target):
    n, blocks = lax.axis_size("ep"), lax.axis_size("corner")

    def place(i, k):
        return (i & ~3 | (i & 1) << 1 | (i >> 1) & 1) if k % 2 else i

    pairs = [(place(i, k) * blocks + k, place(target(i), k) * blocks + k) for i in range(n) for k in range(blocks)]
    return lax.ppermute(value, ("ep", "corner"), pairs)


def tiles(x):
    c, e = x.shape
    return x.reshape(c, e // LANES, LANES).transpose(1, 0, 2).reshape(-1, LANES)


def on_device(required, arrival, hold_required, early_arrival, part_ids, bin_edges):
    C, rows = required.shape
    bins = bin_edges.shape[0]
    n = lax.axis_size("ep")
    me = turned(lax.axis_index("ep"), lax.axis_index("corner") % 2 == 1)
    endpoints = rows * n
    density = GROUPS * bins / endpoints
    half = C // 2
    side = me % 2
    place = me // 2
    rest = n // 2
    data = (tiles(required), tiles(arrival), tiles(early_arrival), tiles(hold_required))
    ids = part_ids.reshape(-1, LANES)
    lines = ids.shape[0]
    coarse, fine, near, keep, send = run_prep(bin_edges, side.reshape(1), ids, *data, C)
    got = moved(send, lambda i: i ^ 1)
    prior = run_hist(place.reshape(1), coarse, fine, keep, half)
    chunks = run_hist(place.reshape(1), coarse, fine, got, half, rest, prior)
    shares = [rotate(near, "corner", d) for d in range(1, lax.axis_size("corner"))]

    own = GROUPS // rest
    nblk = bins // LANES
    each = C * nblk
    hrows = own * each
    total = chunks[0]
    row = lax.broadcasted_iota(jnp.int32, total.shape, 0)
    lane = lax.broadcasted_iota(jnp.int32, total.shape, 1)
    least = (row >= hrows) & (row < hrows + 2 * half) & (lane >= GROUPS)
    order = sorted(range(1, rest), key=lambda d: (d != rest // 2, d))
    for d in order:
        piece = moved(chunks[d], lambda i: i ^ 2 * d)
        total = jnp.where(least, jnp.minimum(total, piece), total + piece)
    mine = jnp.where(row < hrows, total * density, total)
    pieces = [mine] + [None] * (n - 1)
    for d in range(1, rest):
        pieces[2 * d] = moved(mine, lambda i: i ^ 2 * d)
    pieces[1] = moved(mine, lambda i: i ^ 1)
    for d in range(1, rest):
        pieces[2 * d + 1] = moved(pieces[2 * d], lambda i: i ^ 1)
    part_tns, part_share, tns, wns = run_small(me.reshape(1), mine, pieces[1], C, endpoints)
    worst = functools.reduce(jnp.minimum, shares, near)
    worst = worst.reshape(lines, 2, LANES)
    worst = worst.transpose(1, 0, 2).reshape(2, rows)
    full = run_final(me.reshape(1), pieces, own, 2 * each)
    part_hist = full.reshape(GROUPS, C, nblk, 2, LANES).transpose(0, 1, 3, 2, 4).reshape(GROUPS, C, 2, bins)
    part_tns = part_tns.transpose(2, 0, 1)
    part_share = part_share.reshape(GROUPS)
    return (part_hist, part_tns, part_share, tns, wns, worst)


def solution(mesh):
    in_specs = (
        P("corner", "ep"),
        P("corner", "ep"),
        P("corner", "ep"),
        P("corner", "ep"),
        P("ep"),
        P(),
    )
    out_specs = (
        P(None, "corner", None, None),
        P(None, "corner", None),
        P(),
        P("corner", None),
        P("corner", None),
        P(None, "ep"),
    )
    return jax.shard_map(
        on_device, mesh=mesh, in_specs=in_specs, out_specs=out_specs, check_vma=False
    )
```
